32 devices in a mesh: fft: 8 (over z, y), band: 4 (over x, core).
Axes of the slice: x: 2, y: 2, z: 4, core: 2. Of those that a mesh axis runs over, the one named last changes fastest.
Arguments:
- coefficients: bfloat16 [48, 184320], P('band', 'fft'), may hold values from -0.078125 to 0.078125
- occupations: float32 [48], P('band'), may hold values from 0.5 to 2
- columns: int32 [1280], P('fft'), may hold values from 0 to 5183
- counts: int32 [8], P('fft'), may hold values from 1 to 160, 512 in all
- plane_slot: int32 [144], replicated, may hold values from -1 to 143, as said below
Outputs:
- density: float32 [144, 144, 144], P('fft', 'band')
The draws below stay inside these ranges and needn't reach their ends.
Inputs may be any that keep to these rules, and one draw needn't show every extreme that they name: The counts sum to 512, and one of them equals 160. `plane_slot`: every plane 0 .. 143 stands in exactly one slot; the other slots hold -1.
All inputs are finite; a program needn't handle non-finite values. No bound on the sum of `counts` on one device may be relied on, other than what follows from the above.
Results may differ from the reference program's by a relative error of at most 0.0095.
Values may be sent and summed in bfloat16 or wider, within the bound.
No kernel may reach another device: no remote copies, remote signals or barrier semaphores. Data moves between devices by JAX's collectives and lax.ppermute only.
A program may use at most 192 MiB of HBM per device.

```python
import math
import jax
import jax.numpy as jnp
import numpy as np
from jax import lax

N = 144
GB = 72
STICK_DEV = 160
STICKS = 512
STICKS_ALL = 1280
BANDS = 48
SLOTS = 144
N_FFT = 8


def draw_plane_slot(key, part):
    shuffled = jax.random.permutation(key, SLOTS)
    return jnp.where(shuffled < N, shuffled, -1).astype(jnp.int32)


def touch_ends(values, stream_key, least, high):
    longest = values.shape.index(max(values.shape))
    spots = []
    for shift in (0, 1):
        where = [jax.random.randint(jax.random.fold_in(stream_key, axis), (), 0, length) for axis, length in enumerate(values.shape)]
        where[longest] = (where[longest] + shift) % values.shape[longest]
        spots.append(tuple(where))
    return values.at[spots[0]].set(least).at[spots[1]].set(high)


def block_levels(rng, dims, cuts, least, top_value):
    def one(dim, parts):
        draws = jax.random.uniform(jax.random.fold_in(jax.random.fold_in(rng, 6), dim), (parts,), jnp.float32, least / len(cuts), top_value / len(cuts))
        return jnp.repeat(jnp.exp(draws), dims[dim] // parts).reshape((-1,) + (1,) * (len(dims) - dim - 1))

    loudness = one(*cuts[0])
    for cut in cuts[1:]:
        loudness = loudness * one(*cut)
    return loudness


def length_profile(count, total, limit, slope):
    loads = [(1 << 20) // math.isqrt(rank ** slope) + 1 for rank in range(2, count + 1)]
    surplus, given = total - limit - (count - 1), [1] * (count - 1)
    while surplus > 0:
        free = [i for i in range(count - 1) if given[i] < limit]
        mass, budget = sum([loads[i] for i in free]), surplus
        for i in free:
            extra = min(limit - given[i], max(1, budget * loads[i] // mass), surplus)
            given[i] = given[i] + extra
            surplus = surplus - extra
    return np.array([limit] + given)


def ragged_sizes(rng, count, total, reach, slope):
    if count == 2:
        one = jax.random.randint(rng, (), max(1, total - reach), min(reach, total - 1) + 1)
        return jnp.stack([one, total - one])
    lengths = jnp.asarray(length_profile(count, total, reach, slope), jnp.int32)
    twos = (count - 1) // 2
    donor, receiver = lengths[1:1 + 2 * twos:2], lengths[2:2 + 2 * twos:2]
    room = jnp.minimum(donor - 1, reach - receiver)
    shifted = jax.random.randint(jax.random.fold_in(rng, 1), (twos,), 0, 1 << 20) % (room + 1)
    lengths = lengths.at[1:1 + 2 * twos:2].set(donor - shifted).at[2:2 + 2 * twos:2].set(receiver + shifted)
    return lengths[jax.random.permutation(jax.random.fold_in(rng, 2), count)]


def scatter_about(stream_key, shape, width, limit, shards=(), kind=jnp.bfloat16):
    level = block_levels(stream_key, shape, shards, -0.22, 0.18) if shards else 1.0
    entries = jax.random.normal(stream_key, shape, jnp.float32) * width * level
    return jnp.minimum(jnp.maximum(entries, -limit), limit).astype(kind)


def setup_inputs(seed: int = 0) -> dict:
    streams_of = jax.random.split(jax.random.key(seed), 6)
    coefficients = scatter_about(streams_of[0], (BANDS, STICKS_ALL * 2 * GB), (1.0 / (STICKS * GB) ** 0.5), 0.078125, ((0, 4), (1, 8)))
    occupations = jnp.clip(jnp.exp(math.log(2.0) - 1.3862944 * jax.random.uniform(streams_of[1], (BANDS,), jnp.float32) ** block_levels(streams_of[1], (BANDS,), ((0, 4),), -0.2, 0.2)), 0.5, 2.0)
    columns = touch_ends(jax.random.randint(streams_of[2], (STICKS_ALL,), 0, GB * GB), jax.random.fold_in(streams_of[2], 1), 0, (GB * GB) - 1).astype(jnp.int32)
    counts = ragged_sizes(streams_of[3], N_FFT, STICKS, STICK_DEV, 2).astype(jnp.int32)
    plane_slot = draw_plane_slot(jax.random.fold_in(streams_of[5], 71), 0)
    return {"coefficients": coefficients, "occupations": occupations, "columns": columns, "counts": counts, "plane_slot": plane_slot}


def phase_pair(freq_count, positions, grid):
    freqs = jnp.arange(freq_count, dtype=jnp.int32) - freq_count // 2
    turns = jnp.mod(freqs[:, None] * positions[None, :], grid)
    angles = turns.astype(jnp.float32) * (2.0 * math.pi / grid)
    return jnp.cos(angles), jnp.sin(angles)


def stick_table(plane_slot):
    valid_slot = (plane_slot >= 0).astype(jnp.float32)
    cosine, sine_part = phase_pair(GB, jnp.maximum(plane_slot, 0), N)
    cosine = cosine * valid_slot[None, :]
    sine_part = sine_part * valid_slot[None, :]
    upper_rows = jnp.concatenate([cosine, sine_part], axis=1)
    lower_rows = jnp.concatenate([-sine_part, cosine], axis=1)
    return jnp.concatenate([upper_rows, lower_rows], axis=0).astype(jnp.bfloat16)


def row_table():
    cosine, sine_part = phase_pair(GB, jnp.arange(N, dtype=jnp.int32), N)
    upper_rows = jnp.concatenate([cosine, sine_part], axis=1)
    lower_rows = jnp.concatenate([-sine_part, cosine], axis=1)
    return jnp.concatenate([upper_rows, lower_rows], axis=0).astype(jnp.bfloat16)


def column_table():
    cosine, sine_part = phase_pair(GB, jnp.arange(N, dtype=jnp.int32), N)
    return jnp.concatenate([cosine.T, sine_part.T], axis=0).astype(jnp.bfloat16)


def grid_squares(received, real_index, imag_index, row_tab, col_tab):
    bands_here, _, planes, _ = received.shape
    flat_plane = jnp.zeros((bands_here, planes, GB * 2 * GB), jnp.float32)
    flat_plane = flat_plane.at[:, :, real_index].add(received[:, 0].astype(jnp.float32))
    flat_plane = flat_plane.at[:, :, imag_index].add(received[:, 1].astype(jnp.float32))
    g_plane = flat_plane.reshape(bands_here, planes, GB, 2 * GB).astype(jnp.bfloat16)
    half_way = jnp.einsum("bpgk,kj->bpgj", g_plane.astype(jnp.float32), row_tab.astype(jnp.float32)).astype(jnp.bfloat16)
    full_grid = jnp.einsum("xg,bpgj->bpxj", col_tab.astype(jnp.float32), half_way.astype(jnp.float32))
    real_part = full_grid[:, :, :N, :N] - full_grid[:, :, N:, N:]
    imag_part = full_grid[:, :, N:, :N] + full_grid[:, :, :N, N:]
    return real_part * real_part + imag_part * imag_part


def reference(coefficients, occupations, columns, counts, plane_slot):
    shaped = coefficients.reshape(BANDS, STICKS_ALL, 2 * GB)
    stick_place = jnp.arange(STICKS_ALL, dtype=jnp.int32)
    live_stick = (stick_place % STICK_DEV < jnp.repeat(counts, STICK_DEV)).astype(jnp.bfloat16)
    masked = shaped * live_stick[None, :, None]
    real_index = (columns // GB) * (2 * GB) + columns % GB
    imag_index = real_index + GB
    plane_tab = stick_table(plane_slot)
    row_tab = row_table()
    col_tab = column_table()

    def one_band(running, inputs):
        coeffs, weight = inputs
        sticks = jnp.dot(coeffs, plane_tab, preferred_element_type=jnp.float32).astype(jnp.bfloat16)
        outgoing = sticks.T.reshape(1, 2, SLOTS, STICKS_ALL)
        squares = grid_squares(outgoing, real_index, imag_index, row_tab, col_tab)
        return running + weight * squares[0], None

    start = jnp.zeros((SLOTS, N, N), jnp.float32)
    density, _ = lax.scan(one_band, start, (masked, occupations / BANDS))
    return density
```

```python
import functools
import math

import jax
import jax.numpy as jnp
import numpy as np
from jax import lax
from jax.experimental import pallas as pl
from jax.experimental.pallas import tpu as pltpu
from jax.sharding import PartitionSpec as P

N = 144
GB = 72
LANES = 128
TAIL = N - LANES
INFO = 16
GROUPS = 3


def wave_tables():
    freqs = np.arange(GB) - GB // 2
    angles = (freqs[:, None] * np.arange(N)[None, :] % N) * (2.0 * math.pi / N)
    cosine, sine = np.cos(angles), np.sin(angles)
    rows = np.zeros((2 * LANES, 4 * LANES), np.float32)
    for col, real_from, imag_from in ((0, cosine, -sine), (1, sine, cosine)):
        rows[:GB, col * LANES : (col + 1) * LANES] = real_from[:, :LANES]
        rows[LANES : LANES + GB, col * LANES : (col + 1) * LANES] = imag_from[:, :LANES]
        at = (2 + col) * LANES
        rows[:GB, at : at + TAIL] = real_from[:, LANES:]
        rows[LANES : LANES + GB, at : at + TAIL] = imag_from[:, LANES:]
    cols = np.block([[cosine.T, -sine.T], [sine.T, cosine.T]])
    return jnp.asarray(rows, jnp.bfloat16), jnp.asarray(cols, jnp.bfloat16)


def plane_table(plane_slot, chunks, ranks, group):
    held = plane_slot.reshape(ranks, chunks, -1).swapaxes(0, 1)
    planes = held.shape[2]
    held = jnp.concatenate(
        [held, held, jnp.full((chunks, ranks, group - 2 * planes), -1, jnp.int32)], axis=2
    )
    imag_row = jnp.arange(group, dtype=jnp.int32) >= planes
    col = jnp.arange(2 * GB, dtype=jnp.int32)
    imag_col = col >= GB
    freq = col % GB - GB // 2
    quarter = jnp.where(
        imag_row[:, None] == imag_col[None, :], 0, jnp.where(imag_col[None, :], N // 4, 3 * N // 4)
    )
    turns = jnp.mod(freq * jnp.maximum(held, 0)[..., None] + quarter, N)
    table = jnp.cos(turns.astype(jnp.float32) * (2.0 * math.pi / N))
    table = table * (held >= 0).astype(jnp.float32)[..., None]
    return table.reshape(chunks * ranks * group, 2 * GB).astype(jnp.bfloat16)


def lane_group(rows, dtype):
    group = lax.broadcasted_iota(jnp.int32, (rows, LANES), 1) // 32
    return [(group == g).astype(jnp.float32).astype(dtype) for g in range(GROUPS + 1)]


def stick_kernel(bands, chunks, ranks, planes, group, span, coef, tab, info, *refs):
    outs, (main, rest) = refs[:chunks], refs[chunks:]
    live = 2 * planes * bands
    rows = GROUPS * span
    if live < rows:
        main[...] = jnp.zeros_like(main)
        rest[...] = jnp.zeros_like(rest)
    table = tab[...]
    for b in range(bands):
        x = coef[b]
        x = jnp.concatenate([x[:LANES]] + [x[LANES:]] * 4, axis=0)
        val = lax.dot_general(
            table, x, (((1,), (1,)), ((), ())), preferred_element_type=jnp.float32
        )
        for i in range(chunks * ranks):
            part = val[i * group : i * group + 2 * planes]
            main[i, pl.ds(b, 2 * planes, stride=bands), :] = part[:, :LANES]
            rest[i, pl.ds(b, 2 * planes, stride=bands), :] = part[:, LANES:]
    masks = lane_group(span, jnp.float32)
    for i in range(chunks * ranks):
        c, d = divmod(i, ranks)
        outs[c][d, :rows, :] = main[i].astype(jnp.bfloat16)
        packed = rest[i, :span, :] * masks[0]
        for g in range(1, GROUPS):
            packed = packed + rest[i, g * span : (g + 1) * span, :] * masks[g]
        at = rows
        if c == 0:
            outs[c][d, rows : rows + INFO, :] = info[:, :LANES].astype(jnp.bfloat16)
            tail_info = jnp.concatenate(
                [info[:, LANES:], jnp.zeros((span - INFO, LANES), jnp.float32)], axis=0
            )
            packed = packed + tail_info * masks[GROUPS]
            at = rows + INFO
        outs[c][d, at : at + span, :] = packed.astype(jnp.bfloat16)


def plane_kernel(first, bands, ranks, planes, span, owners, own_rows, *refs):
    if first:
        recv, row_tab, col_tab, weight, dens, turn, gx_of, gy_hot = refs[:8]
        scratch = refs[8:]
    else:
        recv, row_tab, col_tab, weight, turn, gx_of, gy_hot, dens = refs[:8]
        scratch = refs[8:]
    lhs, pick, sticks, real, imag, half, tail, acc, acc_tail = scratch
    rows = GROUPS * span
    total = rows + INFO if first else rows
    live = planes * bands
    cap = turn.shape[1]

    if first:
        place = lax.broadcasted_iota(jnp.int32, (1, cap), 1).astype(jnp.float32)
        start = jnp.zeros((1, 1), jnp.float32)
        for src in range(ranks):
            count = recv[src, rows : rows + INFO, :].astype(jnp.float32)[2:3, 0:1]
            t = place - start
            turn[src : src + 1, :] = jnp.where(jnp.logical_and(t >= 0, t < count), t, -1.0)
            start = start + count

    masks = lane_group(span, jnp.bfloat16)
    k = lax.broadcasted_iota(jnp.int32, (2 * LANES, cap), 0)
    slot = jnp.where(k < LANES, k, LANES + k % 32).astype(jnp.float32)
    for src in range(ranks):
        at = src * 2 * LANES
        pick[at : at + 2 * LANES, :] = jnp.where(slot == turn[src : src + 1, :], 1.0, 0.0).astype(
            jnp.bfloat16
        )
        packed = recv[src, total : total + span, :]
        pieces = [packed * masks[g] for g in range(GROUPS)]
        if first:
            pieces.append((packed * masks[GROUPS])[:INFO])
        lhs[:, at : at + LANES] = recv[src, :total, :]
        lhs[:, at + LANES : at + 2 * LANES] = jnp.concatenate(pieces, axis=0)
    compact = jnp.dot(lhs[...], pick[...], preferred_element_type=jnp.float32)
    sticks[...] = compact[:rows].astype(jnp.bfloat16)

    if first:
        info = jnp.concatenate(
            [compact[rows:], jnp.zeros((LANES - INFO, cap), jnp.float32)], axis=0
        ).T
        lane = lax.broadcasted_iota(jnp.int32, (cap, LANES), 1).astype(jnp.float32)
        gx_of[...] = jnp.broadcast_to(info[:, 0:1], (cap, LANES)).astype(jnp.bfloat16)
        gy_hot[...] = jnp.where(info[:, 1:2] == lane, 1.0, 0.0).astype(jnp.bfloat16)

    def put(pair, carry):
        hot = []
        for side in range(2):
            gx = (2 * pair + side).astype(jnp.float32).astype(jnp.bfloat16)
            hot.append(jnp.where(gx_of[...] == gx, gy_hot[...], jnp.zeros((), jnp.bfloat16)))
        placed = jnp.dot(
            sticks[...], jnp.concatenate(hot, axis=1), preferred_element_type=jnp.float32
        )
        for side in range(2):
            lanes = slice(side * LANES, (side + 1) * LANES)
            real[pl.ds(2 * pair + side, live, stride=GB), :] = placed[:live, lanes]
            imag[pl.ds(2 * pair + side, live, stride=GB), :] = placed[live : 2 * live, lanes]
        return carry

    lax.fori_loop(0, GB // 2, put, 0)

    tail[...] = jnp.zeros_like(tail)
    acc[...] = jnp.zeros_like(acc)
    acc_tail[...] = jnp.zeros_like(acc_tail)

    def rows_of(j, carry):
        at = pl.ds(pl.multiple_of(j * (bands * GB), 8), bands * GB)
        both = jnp.concatenate(
            [real[at, :].astype(jnp.bfloat16), imag[at, :].astype(jnp.bfloat16)], axis=1
        )
        h = jnp.dot(both, row_tab[...], preferred_element_type=jnp.float32)
        for b in range(bands):
            piece = h[b * GB : (b + 1) * GB]
            half[j, b] = jnp.concatenate(
                [piece[:, :LANES], piece[:, LANES : 2 * LANES]], axis=0
            ).astype(jnp.bfloat16)
            end = jnp.concatenate(
                [piece[:, 2 * LANES : 3 * LANES], piece[:, 3 * LANES :]], axis=0
            )
            tail[b] = tail[b] + pltpu.roll(end, TAIL * j, 1)
        return carry

    lax.fori_loop(0, planes, rows_of, 0)

    def columns_of(b, carry):
        w = weight[b]

        def square(x):
            wave = jnp.dot(col_tab[...], x, preferred_element_type=jnp.float32)
            a, c = wave[:N], wave[N:]
            return (a * a + c * c) * w

        for j in range(0, planes, 2):
            if j + 1 < planes:
                sq = square(jnp.concatenate([half[j, b], half[j + 1, b]], axis=1))
                acc[j] = acc[j] + sq[:, :LANES]
                acc[j + 1] = acc[j + 1] + sq[:, LANES:]
            else:
                acc[j] = acc[j] + square(half[j, b])
        acc_tail[...] = acc_tail[...] + square(tail[b].astype(jnp.bfloat16))
        return carry

    lax.fori_loop(0, bands, columns_of, 0)

    for o in range(owners):
        mine = slice(o * own_rows, (o + 1) * own_rows)
        for j in range(planes):
            dens[o, j, :own_rows, :] = acc[j, mine, :].astype(jnp.bfloat16)
        dens[o, planes, :own_rows, :] = acc_tail[mine, :].astype(jnp.bfloat16)


def sum_kernel(chunks, owners, planes, own_rows, *refs):
    parts, out = refs[:chunks], refs[chunks]
    for c in range(chunks):
        total = parts[c][0].astype(jnp.float32)
        for o in range(1, owners):
            total = total + parts[c][o].astype(jnp.float32)
        for j in range(planes):
            out[c * planes + j, :, :LANES] = total[j, :own_rows]
            out[c * planes + j, :, LANES:] = total[planes, :own_rows, j * TAIL : (j + 1) * TAIL]


def up(n, m):
    return -(-n // m) * m


def vmem_call(kernel, out_shape, n_in, scratch=(), flops=1, smem=()):
    vmem = pl.BlockSpec(memory_space=pltpu.VMEM)
    scalar = pl.BlockSpec(memory_space=pltpu.SMEM)
    many = isinstance(out_shape, list)
    return pl.pallas_call(
        kernel,
        out_shape=out_shape,
        in_specs=[scalar if i in smem else vmem for i in range(n_in)],
        out_specs=[vmem] * len(out_shape) if many else vmem,
        scratch_shapes=list(scratch),
        compiler_params=pltpu.CompilerParams(vmem_limit_bytes=60 * 2**20),
        cost_estimate=pl.CostEstimate(flops=flops, bytes_accessed=1 << 20, transcendentals=0),
    )


def shards(coefficients, occupations, columns, counts, plane_slot):
    bands = coefficients.shape[0]
    ranks = lax.axis_size("fft")
    owners = lax.axis_size("band")
    slots = columns.shape[0]
    held = plane_slot.shape[0] // ranks
    chunks = next(c for c in range(1, held + 1) if held % c == 0 and held // c * TAIL <= LANES)
    planes = held // chunks
    group = up(2 * planes, 16)
    span = up(-(-2 * planes * bands // GROUPS), 16)
    rows = GROUPS * span
    cap = up(ranks * slots * 2 // 5, LANES)
    own_rows = N // owners
    bf16, f32 = jnp.bfloat16, jnp.float32

    coef = coefficients.reshape(bands, slots, 2 * GB)
    table = plane_table(plane_slot, chunks, ranks, group)
    spread = jnp.concatenate([columns[:LANES]] + [columns[LANES:]] * 4)
    row = jnp.arange(INFO, dtype=jnp.int32)[:, None]
    info = jnp.where(
        row == 0, spread // GB, jnp.where(row == 1, spread % GB, jnp.where(row == 2, counts[0], 0))
    ).astype(f32)
    weight = occupations / (bands * owners)
    row_tab, col_tab = wave_tables()

    shapes = [
        jax.ShapeDtypeStruct((ranks, rows + span + (INFO if c == 0 else 0), LANES), bf16)
        for c in range(chunks)
    ]
    outgoing = vmem_call(
        functools.partial(stick_kernel, bands, chunks, ranks, planes, group, span),
        shapes,
        3,
        [pltpu.VMEM((chunks * ranks, rows, LANES), f32)] * 2,
        flops=4 * 10**9,
    )(coef, table, info)
    dens_shape = jax.ShapeDtypeStruct((owners, planes + 1, up(own_rows, 8), LANES), bf16)
    kept_shapes = [
        jax.ShapeDtypeStruct((ranks, cap), f32),
        jax.ShapeDtypeStruct((cap, LANES), bf16),
        jax.ShapeDtypeStruct((cap, LANES), bf16),
    ]
    kept, summed = [], []
    for c in range(chunks):
        first = c == 0
        received = lax.all_to_all(outgoing[c], "fft", split_axis=0, concat_axis=0, tiled=True)
        total = rows + (INFO if first else 0)
        results = vmem_call(
            functools.partial(plane_kernel, first, bands, ranks, planes, span, owners, own_rows),
            [dens_shape] + (kept_shapes if first else []),
            4 if first else 7,
            [
                pltpu.VMEM((total, ranks * 2 * LANES), bf16),
                pltpu.VMEM((ranks * 2 * LANES, cap), bf16),
                pltpu.VMEM((rows, cap), bf16),
                pltpu.VMEM((planes * bands * GB, LANES), f32),
                pltpu.VMEM((planes * bands * GB, LANES), f32),
                pltpu.VMEM((planes, bands, 2 * GB, LANES), bf16),
                pltpu.VMEM((bands, 2 * GB, LANES), f32),
                pltpu.VMEM((planes, N, LANES), f32),
                pltpu.VMEM((N, LANES), f32),
            ],
            flops=16 * 10**9,
            smem=(3,),
        )(received, row_tab, col_tab, weight, *kept)
        if first:
            kept = list(results[1:])
        summed.append(
            lax.all_to_all(results[0], "band", split_axis=0, concat_axis=0, tiled=True)
        )
    return vmem_call(
        functools.partial(sum_kernel, chunks, owners, planes, own_rows),
        jax.ShapeDtypeStruct((held, own_rows, N), f32),
        chunks,
    )(*summed)


def solution(mesh):
    placed = (P("band", "fft"), P("band"), P("fft"), P("fft"), P())
    return jax.shard_map(
        shards, mesh=mesh, in_specs=placed, out_specs=P("fft", "band", None), check_vma=False
    )
```

```python
import functools
import math

import jax
import jax.numpy as jnp
import numpy as np
from jax import lax
from jax.experimental import pallas as pl
from jax.experimental.pallas import tpu as pltpu
from jax.sharding import PartitionSpec as P

N = 144
GB = 72
LANES = 128
TAIL = N - LANES
SHARE = LANES // TAIL
PAIRS = 4
INFO = 16
GROUPS = 3


def wave_tables():
    freqs = np.arange(GB) - GB // 2
    angles = (freqs[:, None] * np.arange(N)[None, :] % N) * (2.0 * math.pi / N)
    cosine, sine = np.cos(angles), np.sin(angles)
    rows = np.zeros((2 * LANES, 2 * LANES), np.float32)
    ends = np.zeros((SHARE, 2 * LANES, 2 * LANES), np.float32)
    for col, real_from, imag_from in ((0, cosine, -sine), (1, sine, cosine)):
        rows[:GB, col * LANES : (col + 1) * LANES] = real_from[:, :LANES]
        rows[LANES : LANES + GB, col * LANES : (col + 1) * LANES] = imag_from[:, :LANES]
        for j in range(SHARE):
            at = col * LANES + j * TAIL
            ends[j, :GB, at : at + TAIL] = real_from[:, LANES:]
            ends[j, LANES : LANES + GB, at : at + TAIL] = imag_from[:, LANES:]
    cols = np.block([[cosine.T, -sine.T], [sine.T, cosine.T]])
    ends = ends.reshape(SHARE * 2 * LANES, 2 * LANES)
    return [jnp.asarray(x, jnp.bfloat16) for x in (rows, ends, cols)]


def plane_table(plane_slot, planes, ranks):
    held = plane_slot.reshape(ranks, -1)
    rows, imag_rows, base = [], [], 0
    for count in planes:
        group = up(2 * count, 16)
        part = held[:, base : base + count]
        empty = jnp.full((ranks, group - 2 * count), -1, jnp.int32)
        rows.append(jnp.concatenate([part, part, empty], axis=1).reshape(-1))
        imag_rows.append(np.tile(np.arange(group) >= count, ranks))
        base += count
    held = jnp.concatenate(rows)[:, None]
    imag_row = np.concatenate(imag_rows)[:, None]
    col = np.arange(2 * GB)
    imag_col = (col >= GB)[None, :]
    freq = col % GB - GB // 2
    quarter = np.where(imag_row == imag_col, 0, np.where(imag_col, N // 4, 3 * N // 4))
    turns = jnp.mod(freq * jnp.maximum(held, 0) + quarter.astype(np.int32), N)
    table = jnp.cos(turns.astype(jnp.float32) * (2.0 * math.pi / N))
    return jnp.where(held >= 0, table, 0.0).astype(jnp.bfloat16)


def lane_group(rows, dtype):
    group = lax.broadcasted_iota(jnp.int32, (rows, LANES), 1) // 32
    return [(group == g).astype(jnp.float32).astype(dtype) for g in range(GROUPS + 1)]


def stick_kernel(bands, planes, ranks, coef, tab, info, *refs):
    chunks = len(planes)
    outs, mains, rests = refs[:chunks], refs[chunks : 2 * chunks], refs[2 * chunks :]
    for main, rest, count in zip(mains, rests, planes):
        if 2 * count * bands < main.shape[1]:
            main[...] = jnp.zeros_like(main)
            rest[...] = jnp.zeros_like(rest)
    table = tab[...]
    for b in range(bands):
        x = coef[b]
        x = jnp.concatenate([x[:LANES]] + [x[LANES:]] * 4, axis=0)
        val = lax.dot_general(
            table, x, (((1,), (1,)), ((), ())), preferred_element_type=jnp.float32
        )
        at = 0
        for main, rest, count in zip(mains, rests, planes):
            for d in range(ranks):
                part = val[at : at + 2 * count]
                main[d, pl.ds(b, 2 * count, stride=bands), :] = part[:, :LANES]
                rest[d, pl.ds(b, 2 * count, stride=bands), :] = part[:, LANES:]
                at += up(2 * count, 16)
    for c, (out, main, rest) in enumerate(zip(outs, mains, rests)):
        rows = main.shape[1]
        span = rows // GROUPS
        masks = lane_group(span, jnp.float32)
        at = rows + (INFO if c == 0 else 0)
        for d in range(ranks):
            out[d, :rows, :] = main[d].astype(jnp.bfloat16)
            packed = rest[d, :span, :] * masks[0]
            for g in range(1, GROUPS):
                packed = packed + rest[d, g * span : (g + 1) * span, :] * masks[g]
            if c == 0:
                out[d, rows:at, :] = info[:, :LANES].astype(jnp.bfloat16)
                tail_info = jnp.concatenate(
                    [info[:, LANES:], jnp.zeros((span - INFO, LANES), jnp.float32)], axis=0
                )
                packed = packed + tail_info * masks[GROUPS]
            out[d, at:, :] = packed.astype(jnp.bfloat16)


def plane_kernel(first, bands, ranks, planes, span, owners, own_rows, *refs):
    if first:
        recv, row_tab, end_tab, col_tab, weight, dens, turn, gx_of, gy_hot = refs[:9]
    else:
        recv, row_tab, end_tab, col_tab, weight, turn, gx_of, gy_hot, dens = refs[:9]
    lhs, pick, sticks, real, imag, both, half, tail, acc, acc_tail = refs[9:]
    rows = GROUPS * span
    total = rows + INFO if first else rows
    live = planes * bands
    cap = turn.shape[1]

    if first:
        place = lax.broadcasted_iota(jnp.int32, (1, cap), 1).astype(jnp.float32)
        start = jnp.zeros((1, 1), jnp.float32)
        for src in range(ranks):
            count = recv[src, rows : rows + INFO, :].astype(jnp.float32)[2:3, 0:1]
            t = place - start
            turn[src : src + 1, :] = jnp.where(jnp.logical_and(t >= 0, t < count), t, -1.0)
            start = start + count

    masks = lane_group(span, jnp.bfloat16)
    k = lax.broadcasted_iota(jnp.int32, (2 * LANES, cap), 0)
    slot = jnp.where(k < LANES, k, LANES + k % 32).astype(jnp.float32)
    for src in range(ranks):
        at = src * 2 * LANES
        pick[at : at + 2 * LANES, :] = jnp.where(slot == turn[src : src + 1, :], 1.0, 0.0).astype(
            jnp.bfloat16
        )
        packed = recv[src, total : total + span, :]
        pieces = [packed * masks[g] for g in range(GROUPS)]
        if first:
            pieces.append((packed * masks[GROUPS])[:INFO])
        lhs[:, at : at + LANES] = recv[src, :total, :]
        lhs[:, at + LANES : at + 2 * LANES] = jnp.concatenate(pieces, axis=0)
    compact = jnp.dot(lhs[...], pick[...], preferred_element_type=jnp.float32)
    sticks[...] = compact[:rows].astype(jnp.bfloat16)

    if first:
        info = jnp.concatenate(
            [compact[rows:], jnp.zeros((LANES - INFO, cap), jnp.float32)], axis=0
        ).T
        lane = lax.broadcasted_iota(jnp.int32, (cap, LANES), 1).astype(jnp.float32)
        gx_of[...] = jnp.broadcast_to(info[:, 0:1], (cap, LANES)).astype(jnp.bfloat16)
        gy_hot[...] = jnp.where(info[:, 1:2] == lane, 1.0, 0.0).astype(jnp.bfloat16)

    def put(step, carry):
        for u in range(PAIRS):
            pair = PAIRS * step + u
            hot = []
            for side in range(2):
                gx = (2 * pair + side).astype(jnp.float32).astype(jnp.bfloat16)
                hot.append(jnp.where(gx_of[...] == gx, gy_hot[...], jnp.zeros((), jnp.bfloat16)))
            placed = jnp.dot(
                sticks[...], jnp.concatenate(hot, axis=1), preferred_element_type=jnp.float32
            )
            for side in range(2):
                lanes = slice(side * LANES, (side + 1) * LANES)
                at = 2 * pair + side
                real[pl.ds(at, live, stride=GB), :] = placed[:live, lanes]
                imag[pl.ds(at, live, stride=GB), :] = placed[live : 2 * live, lanes]
        return carry

    lax.fori_loop(0, GB // 2 // PAIRS, put, 0)

    acc[...] = jnp.zeros_like(acc)
    acc_tail[...] = jnp.zeros_like(acc_tail)

    def stacked(piece):
        return jnp.concatenate([piece[:, :LANES], piece[:, LANES:]], axis=0).astype(jnp.bfloat16)

    def rows_of(j, carry):
        at = pl.ds(pl.multiple_of(j * (bands * GB), 8), bands * GB)
        x = jnp.concatenate(
            [real[at, :].astype(jnp.bfloat16), imag[at, :].astype(jnp.bfloat16)], axis=1
        )
        both[j] = x
        h = jnp.dot(x, row_tab[...], preferred_element_type=jnp.float32)
        for b in range(bands):
            half[j, b] = stacked(h[b * GB : (b + 1) * GB])
        return carry

    lax.fori_loop(0, planes, rows_of, 0)

    tails = tail.shape[0]
    for t in range(tails):
        js = range(t * SHARE, min(planes, (t + 1) * SHARE))
        x = jnp.concatenate([both[j] for j in js], axis=1)
        h = jnp.dot(x, end_tab[: len(js) * 2 * LANES, :], preferred_element_type=jnp.float32)
        for b in range(bands):
            tail[t, b] = stacked(h[b * GB : (b + 1) * GB])

    def columns_of(step, carry):
        for u in range(2):
            b = 2 * step + u
            w = weight[b]
            pieces = [(acc, j, half) for j in range(planes)]
            pieces += [(acc_tail, t, tail) for t in range(tails)]
            for i in range(0, len(pieces), 2):
                two = pieces[i : i + 2]
                x = jnp.concatenate([src[j, b] for _, j, src in two], axis=1)
                wave = jnp.dot(col_tab[...], x, preferred_element_type=jnp.float32)
                re, im = wave[:N], wave[N:]
                sq = (re * re + im * im) * w
                for side, (to, j, _) in enumerate(two):
                    to[j] = to[j] + sq[:, side * LANES : (side + 1) * LANES]
        return carry

    lax.fori_loop(0, bands // 2, columns_of, 0)

    for o in range(owners):
        mine = slice(o * own_rows, (o + 1) * own_rows)
        for j in range(planes):
            dens[o, j, :own_rows, :] = acc[j, mine, :].astype(jnp.bfloat16)
        for t in range(tails):
            dens[o, planes + t, :own_rows, :] = acc_tail[t, mine, :].astype(jnp.bfloat16)


def sum_kernel(planes, own_rows, *refs):
    *parts, out = refs
    base = 0
    for c, count in enumerate(planes):
        total = parts[2 * c][...].astype(jnp.float32) + parts[2 * c + 1][...].astype(jnp.float32)
        for j in range(count):
            at = j % SHARE * TAIL
            out[base + j, :, :LANES] = total[j, :own_rows]
            out[base + j, :, LANES:] = total[count + j // SHARE, :own_rows, at : at + TAIL]
        base += count


def up(n, m):
    return -(-n // m) * m


def vmem_call(kernel, out_shape, n_in, scratch=(), flops=1, smem=()):
    vmem = pl.BlockSpec(memory_space=pltpu.VMEM)
    scalar = pl.BlockSpec(memory_space=pltpu.SMEM)
    many = isinstance(out_shape, list)
    return pl.pallas_call(
        kernel,
        out_shape=out_shape,
        in_specs=[scalar if i in smem else vmem for i in range(n_in)],
        out_specs=[vmem] * len(out_shape) if many else vmem,
        scratch_shapes=list(scratch),
        compiler_params=pltpu.CompilerParams(vmem_limit_bytes=60 * 2**20),
        cost_estimate=pl.CostEstimate(flops=flops, bytes_accessed=1 << 20, transcendentals=0),
    )


def halve(whole, axis):
    bit = 0
    while True:
        here = lax.axis_index(axis) >> bit & 1
        pairs = whole.reshape((whole.shape[0] // 2, 2) + whole.shape[1:])
        keep = lax.dynamic_index_in_dim(pairs, here, 1, keepdims=False)
        send = lax.dynamic_index_in_dim(pairs, 1 - here, 1, keepdims=False)
        partners = [(i, i ^ (1 << bit)) for i in range(lax.axis_size(axis))]
        got = lax.ppermute(send, axis, partners)
        if keep.shape[0] == 1:
            return keep[0], got[0]
        whole = (keep.astype(jnp.float32) + got.astype(jnp.float32)).astype(whole.dtype)
        bit += 1


def shards(coefficients, occupations, columns, counts, plane_slot):
    bands = coefficients.shape[0]
    ranks = lax.axis_size("fft")
    owners = lax.axis_size("band")
    slots = columns.shape[0]
    held = plane_slot.shape[0] // ranks
    planes = (held - held // 3, held // 3)
    cap = up(ranks * slots * 2 // 5, LANES)
    own_rows = N // owners
    bf16, f32 = jnp.bfloat16, jnp.float32

    coef = coefficients.reshape(bands, slots, 2 * GB)
    table = plane_table(plane_slot, planes, ranks)
    spread = jnp.concatenate([columns[:LANES]] + [columns[LANES:]] * 4)
    row = jnp.arange(INFO, dtype=jnp.int32)[:, None]
    info = jnp.where(
        row == 0, spread // GB, jnp.where(row == 1, spread % GB, jnp.where(row == 2, counts[0], 0))
    ).astype(f32)
    weight = occupations / (bands * owners)
    tables = wave_tables()

    spans = [up(-(-2 * count * bands // GROUPS), 16) for count in planes]
    outgoing = vmem_call(
        functools.partial(stick_kernel, bands, planes, ranks),
        [
            jax.ShapeDtypeStruct((ranks, 4 * span + (INFO if c == 0 else 0), LANES), bf16)
            for c, span in enumerate(spans)
        ],
        3,
        [pltpu.VMEM((ranks, GROUPS * span, LANES), f32) for span in spans * 2],
        flops=4 * 10**9,
    )(coef, table, info)
    kept_shapes = [
        jax.ShapeDtypeStruct((ranks, cap), f32),
        jax.ShapeDtypeStruct((cap, LANES), bf16),
        jax.ShapeDtypeStruct((cap, LANES), bf16),
    ]
    kept, halves = [], []
    for c, (count, span) in enumerate(zip(planes, spans)):
        first = c == 0
        received = lax.all_to_all(outgoing[c], "fft", split_axis=0, concat_axis=0, tiled=True)
        rows = GROUPS * span
        tails = -(-count // SHARE)
        dens_shape = jax.ShapeDtypeStruct((owners, count + tails, up(own_rows, 8), LANES), bf16)
        results = vmem_call(
            functools.partial(plane_kernel, first, bands, ranks, count, span, owners, own_rows),
            [dens_shape] + (kept_shapes if first else []),
            5 if first else 8,
            [
                pltpu.VMEM((rows + (INFO if first else 0), ranks * 2 * LANES), bf16),
                pltpu.VMEM((ranks * 2 * LANES, cap), bf16),
                pltpu.VMEM((rows, cap), bf16),
                pltpu.VMEM((count * bands * GB, LANES), f32),
                pltpu.VMEM((count * bands * GB, LANES), f32),
                pltpu.VMEM((count, bands * GB, 2 * LANES), bf16),
                pltpu.VMEM((count, bands, 2 * GB, LANES), bf16),
                pltpu.VMEM((tails, bands, 2 * GB, LANES), bf16),
                pltpu.VMEM((count, N, LANES), f32),
                pltpu.VMEM((tails, N, LANES), f32),
            ],
            flops=16 * 10**9,
            smem=(4,),
        )(received, *tables, weight, *kept)
        if first:
            kept = list(results[1:])
        halves += halve(results[0], "band")
    return vmem_call(
        functools.partial(sum_kernel, planes, own_rows),
        jax.ShapeDtypeStruct((held, own_rows, N), f32),
        len(halves),
    )(*halves)


def solution(mesh):
    placed = (P("band", "fft"), P("band"), P("fft"), P("fft"), P())
    return jax.shard_map(
        shards, mesh=mesh, in_specs=placed, out_specs=P("fft", "band", None), check_vma=False
    )
```

```python
import functools
import math

import jax
import jax.numpy as jnp
import numpy as np
from jax import lax
from jax.experimental import pallas as pl
from jax.experimental.pallas import tpu as pltpu
from jax.sharding import PartitionSpec as P


N = 144
GB = 72
LANES = 128
TAIL = N - LANES
SHARE = LANES // TAIL
PAIRS = 12
INFO = 16
GROUPS = 3


def wave_tables():
    freqs = np.arange(GB) - GB // 2
    angles = (freqs[:, None] * np.arange(N)[None, :] % N) * (2.0 * math.pi / N)
    cosine, sine = np.cos(angles), np.sin(angles)
    rows = np.zeros((2 * LANES, 2 * LANES), np.float32)
    ends = np.zeros((SHARE, 2 * LANES, 2 * LANES), np.float32)
    for col, real_from, imag_from in ((0, cosine, -sine), (1, sine, cosine)):
        rows[:GB, col * LANES : (col + 1) * LANES] = real_from[:, :LANES]
        rows[LANES : LANES + GB, col * LANES : (col + 1) * LANES] = imag_from[:, :LANES]
        for j in range(SHARE):
            at = col * LANES + j * TAIL
            ends[j, :GB, at : at + TAIL] = real_from[:, LANES:]
            ends[j, LANES : LANES + GB, at : at + TAIL] = imag_from[:, LANES:]
    cols = np.block([[cosine.T, -sine.T], [sine.T, cosine.T]])
    ends = ends.reshape(SHARE * 2 * LANES, 2 * LANES)
    return [jnp.asarray(x, jnp.bfloat16) for x in (rows, ends, cols)]


def plane_table(plane_slot, planes, ranks):
    held = plane_slot.reshape(ranks, -1)
    rows, imag_rows, base = [], [], 0
    for count in planes:
        group = up(2 * count, 8)
        part = held[:, base : base + count]
        empty = jnp.full((ranks, group - 2 * count), -1, jnp.int32)
        rows.append(jnp.concatenate([part, part, empty], axis=1).reshape(-1))
        imag_rows.append(np.tile(np.arange(group) >= count, ranks))
        base += count
    held = jnp.concatenate(rows)[:, None]
    imag_row = np.concatenate(imag_rows)[:, None]
    col = np.arange(2 * GB)
    imag_col = (col >= GB)[None, :]
    freq = col % GB - GB // 2
    quarter = np.where(imag_row == imag_col, 0, np.where(imag_col, N // 4, 3 * N // 4))
    turns = jnp.mod(freq * jnp.maximum(held, 0) + quarter.astype(np.int32), N)
    table = jnp.cos(turns.astype(jnp.float32) * (2.0 * math.pi / N))
    return jnp.where(held >= 0, table, 0.0).astype(jnp.bfloat16)


def lane_group(rows, dtype):
    group = lax.broadcasted_iota(jnp.int32, (rows, LANES), 1) // 32
    return [(group == g).astype(jnp.float32).astype(dtype) for g in range(GROUPS + 1)]


def stick_kernel(bands, planes, ranks, coef, tab, info, *refs):
    chunks = len(planes)
    outs, mains, rests = refs[:chunks], refs[chunks : 2 * chunks], refs[2 * chunks :]
    for main, rest, count in zip(mains, rests, planes):
        if 2 * count * bands < main.shape[1]:
            main[...] = jnp.zeros_like(main)
            rest[...] = jnp.zeros_like(rest)
    table = tab[...]
    for b in range(bands):
        x = coef[b]
        x = jnp.concatenate([x[:LANES]] + [x[LANES:]] * 4, axis=0)
        val = lax.dot_general(
            table, x, (((1,), (1,)), ((), ())), preferred_element_type=jnp.float32
        )
        at = 0
        for main, rest, count in zip(mains, rests, planes):
            for d in range(ranks):
                part = val[at : at + 2 * count]
                main[d, pl.ds(b, 2 * count, stride=bands), :] = part[:, :LANES]
                rest[d, pl.ds(b, 2 * count, stride=bands), :] = part[:, LANES:]
                at += up(2 * count, 8)
    for c, (out, main, rest) in enumerate(zip(outs, mains, rests)):
        rows = main.shape[1]
        span = rows // GROUPS
        masks = lane_group(span, jnp.float32)
        at = rows + (INFO if c == 0 else 0)
        for d in range(ranks):
            out[d, :rows, :] = main[d].astype(jnp.bfloat16)
            packed = rest[d, :span, :] * masks[0]
            for g in range(1, GROUPS):
                packed = packed + rest[d, g * span : (g + 1) * span, :] * masks[g]
            if c == 0:
                out[d, rows:at, :] = info[:, :LANES].astype(jnp.bfloat16)
                tail_info = jnp.concatenate(
                    [info[:, LANES:], jnp.zeros((span - INFO, LANES), jnp.float32)], axis=0
                )
                packed = packed + tail_info * masks[GROUPS]
            out[d, at:, :] = packed.astype(jnp.bfloat16)


def plane_kernel(first, bands, ranks, planes, span, owners, own_rows, *refs):
    if first:
        recv, row_tab, end_tab, col_tab, weight, core, keep, send, turn, gx_of, gy_hot = refs[:11]
    else:
        recv, row_tab, end_tab, col_tab, weight, core, turn, gx_of, gy_hot, keep, send = refs[:11]
    lhs, pick, sticks, real, imag, both, half, tail, acc, acc_tail = refs[11:]
    rows = GROUPS * span
    total = rows + INFO if first else rows
    live = planes * bands
    cap = turn.shape[1]

    if first:
        place = lax.broadcasted_iota(jnp.int32, (1, cap), 1).astype(jnp.float32)
        start = jnp.zeros((1, 1), jnp.float32)
        for src in range(ranks):
            count = recv[src, rows : rows + INFO, :].astype(jnp.float32)[2:3, 0:1]
            t = place - start
            turn[src : src + 1, :] = jnp.where(jnp.logical_and(t >= 0, t < count), t, -1.0)
            start = start + count

    masks = lane_group(span, jnp.bfloat16)
    k = lax.broadcasted_iota(jnp.int32, (2 * LANES, cap), 0)
    slot = jnp.where(k < LANES, k, LANES + k % 32).astype(jnp.float32)
    for src in range(ranks):
        at = src * 2 * LANES
        pick[at : at + 2 * LANES, :] = jnp.where(slot == turn[src : src + 1, :], 1.0, 0.0).astype(
            jnp.bfloat16
        )
        packed = recv[src, total : total + span, :]
        pieces = [packed * masks[g] for g in range(GROUPS)]
        if first:
            pieces.append((packed * masks[GROUPS])[:INFO])
        lhs[:, at : at + LANES] = recv[src, :total, :]
        lhs[:, at + LANES : at + 2 * LANES] = jnp.concatenate(pieces, axis=0)
    compact = jnp.dot(lhs[...], pick[...], preferred_element_type=jnp.float32)
    sticks[...] = compact[:rows].astype(jnp.bfloat16)

    if first:
        info = jnp.concatenate(
            [compact[rows:], jnp.zeros((LANES - INFO, cap), jnp.float32)], axis=0
        ).T
        lane = lax.broadcasted_iota(jnp.int32, (cap, LANES), 1).astype(jnp.float32)
        gx_of[...] = jnp.broadcast_to(info[:, 0:1], (cap, LANES)).astype(jnp.bfloat16)
        gy_hot[...] = jnp.where(info[:, 1:2] == lane, 1.0, 0.0).astype(jnp.bfloat16)

    def put(step, carry):
        for u in range(PAIRS):
            pair = PAIRS * step + u
            hot = []
            for side in range(2):
                gx = (2 * pair + side).astype(jnp.float32).astype(jnp.bfloat16)
                hot.append(jnp.where(gx_of[...] == gx, gy_hot[...], jnp.zeros((), jnp.bfloat16)))
            placed = jnp.dot(
                sticks[...], jnp.concatenate(hot, axis=1), preferred_element_type=jnp.float32
            )
            for side in range(2):
                lanes = slice(side * LANES, (side + 1) * LANES)
                at = 2 * pair + side
                real[pl.ds(at, live, stride=GB), :] = placed[:live, lanes]
                imag[pl.ds(at, live, stride=GB), :] = placed[live : 2 * live, lanes]
        return carry

    lax.fori_loop(0, GB // 2 // PAIRS, put, 0)

    acc[...] = jnp.zeros_like(acc)
    acc_tail[...] = jnp.zeros_like(acc_tail)

    def stacked(piece):
        return jnp.concatenate([piece[:, :LANES], piece[:, LANES:]], axis=0).astype(jnp.bfloat16)

    def rows_of(step, carry):
        for u in range(deep):
            j = step * deep + u
            at = pl.ds(pl.multiple_of(j * (bands * GB), 8), bands * GB)
            x = jnp.concatenate(
                [real[at, :].astype(jnp.bfloat16), imag[at, :].astype(jnp.bfloat16)], axis=1
            )
            both[j] = x
            h = jnp.dot(x, row_tab[...], preferred_element_type=jnp.float32)
            for b in range(bands):
                half[j, b] = stacked(h[b * GB : (b + 1) * GB])
        return carry

    deep = largest(planes, 3)
    lax.fori_loop(0, planes // deep, rows_of, 0)

    tails = tail.shape[0]
    for t in range(tails):
        js = range(t * SHARE, min(planes, (t + 1) * SHARE))
        x = jnp.concatenate([both[j] for j in js], axis=1)
        h = jnp.dot(x, end_tab[: len(js) * 2 * LANES, :], preferred_element_type=jnp.float32)
        for b in range(bands):
            tail[t, b] = stacked(h[b * GB : (b + 1) * GB])

    wide = largest(bands, 4)

    def columns_of(step, carry):
        pieces = []
        for u in range(wide):
            b = wide * step + u
            pieces += [(acc, j, half, b) for j in range(planes)]
        for t in range(tails):
            pieces += [(acc_tail, t, tail, wide * step + u) for u in range(wide)]
        for i in range(0, len(pieces), 2):
            two = pieces[i : i + 2]
            x = jnp.concatenate([src[j, b] for _, j, src, b in two], axis=1)
            wave = jnp.dot(col_tab[...], x, preferred_element_type=jnp.float32)
            re, im = wave[:N], wave[N:]
            sq = re * re + im * im
            for side, (to, j, _, b) in enumerate(two):
                to[j] = to[j] + sq[:, side * LANES : (side + 1) * LANES] * weight[b]
        return carry

    lax.fori_loop(0, bands // wide, columns_of, 0)

    def deal(mine_bit):
        for o in range(owners):
            to = keep if o % 2 == mine_bit else send
            mine = slice(o * own_rows, (o + 1) * own_rows)
            for j in range(planes):
                to[o // 2, j, :own_rows, :] = acc[j, mine, :].astype(jnp.bfloat16)
            for t in range(tails):
                to[o // 2, planes + t, :own_rows, :] = acc_tail[t, mine, :].astype(jnp.bfloat16)

    @pl.when(core[0] == 0)
    def _():
        deal(0)

    @pl.when(core[0] != 0)
    def _():
        deal(1)


def sum_kernel(planes, own_rows, *refs):
    *parts, out = refs
    base = 0
    for c, count in enumerate(planes):
        total = parts[2 * c][...].astype(jnp.float32) + parts[2 * c + 1][...].astype(jnp.float32)
        for j in range(count):
            at = j % SHARE * TAIL
            out[base + j, :, :LANES] = total[j, :own_rows]
            out[base + j, :, LANES:] = total[count + j // SHARE, :own_rows, at : at + TAIL]
        base += count


def up(n, m):
    return -(-n // m) * m


def largest(n, most):
    return max(d for d in range(1, most + 1) if n % d == 0)


def vmem_call(kernel, out_shape, n_in, scratch=(), flops=1, smem=()):
    used = sum(math.prod(m.shape) * jnp.dtype(m.dtype).itemsize for m in scratch)
    vmem = pl.BlockSpec(memory_space=pltpu.VMEM)
    scalar = pl.BlockSpec(memory_space=pltpu.SMEM)
    many = isinstance(out_shape, list)
    return pl.pallas_call(
        kernel,
        out_shape=out_shape,
        in_specs=[scalar if i in smem else vmem for i in range(n_in)],
        out_specs=[vmem] * len(out_shape) if many else vmem,
        scratch_shapes=list(scratch),
        compiler_params=pltpu.CompilerParams(vmem_limit_bytes=min(63 * 2**20, used + 12 * 2**20)),
        cost_estimate=pl.CostEstimate(flops=flops, bytes_accessed=1 << 20, transcendentals=0),
    )


def partners(axis, bit):
    return [(i, i ^ (1 << bit)) for i in range(lax.axis_size(axis))]


def halve(keep, send, axis):
    bit = 0
    while True:
        got = lax.ppermute(send, axis, partners(axis, bit))
        if keep.shape[0] == 1:
            return keep[0], got[0]
        whole = (keep.astype(jnp.float32) + got.astype(jnp.float32)).astype(keep.dtype)
        bit += 1
        here = lax.axis_index(axis) >> bit & 1
        pairs = whole.reshape((whole.shape[0] // 2, 2) + whole.shape[1:])
        keep = lax.dynamic_index_in_dim(pairs, here, 1, keepdims=False)
        send = lax.dynamic_index_in_dim(pairs, 1 - here, 1, keepdims=False)


def shards(coefficients, occupations, columns, counts, plane_slot):
    bands = coefficients.shape[0]
    ranks = lax.axis_size("fft")
    owners = lax.axis_size("band")
    slots = columns.shape[0]
    held = plane_slot.shape[0] // ranks
    last = min(SHARE, held // 2)
    planes = (held - last, last)
    cap = up(ranks * slots * 2 // 5, LANES)
    own_rows = N // owners
    bf16, f32 = jnp.bfloat16, jnp.float32

    coef = coefficients.reshape(bands, slots, 2 * GB)
    table = plane_table(plane_slot, planes, ranks)
    spread = jnp.concatenate([columns[:LANES]] + [columns[LANES:]] * 4)
    row = jnp.arange(INFO, dtype=jnp.int32)[:, None]
    info = jnp.where(
        row == 0, spread // GB, jnp.where(row == 1, spread % GB, jnp.where(row == 2, counts[0], 0))
    ).astype(f32)
    weight = occupations / (bands * owners)
    core = (lax.axis_index("band") & 1)[None]
    tables = wave_tables()

    spans = [up(-(-2 * count * bands // GROUPS), 16) for count in planes]
    outgoing = vmem_call(
        functools.partial(stick_kernel, bands, planes, ranks),
        [
            jax.ShapeDtypeStruct((ranks, 4 * span + (INFO if c == 0 else 0), LANES), bf16)
            for c, span in enumerate(spans)
        ],
        3,
        [pltpu.VMEM((ranks, GROUPS * span, LANES), f32) for span in spans * 2],
        flops=4 * 10**9,
    )(coef, table, info)
    kept_shapes = [
        jax.ShapeDtypeStruct((ranks, cap), f32),
        jax.ShapeDtypeStruct((cap, LANES), bf16),
        jax.ShapeDtypeStruct((cap, LANES), bf16),
    ]
    kept, halves = [], []
    for c, (count, span) in enumerate(zip(planes, spans)):
        first = c == 0
        received = lax.all_to_all(outgoing[c], "fft", split_axis=0, concat_axis=0, tiled=True)
        rows = GROUPS * span
        tails = -(-count // SHARE)
        dens_shape = jax.ShapeDtypeStruct(
            (owners // 2, count + tails, up(own_rows, 8), LANES), bf16
        )
        run = vmem_call(
            functools.partial(plane_kernel, first, bands, ranks, count, span, owners, own_rows),
            [dens_shape] * 2 + (kept_shapes if first else []),
            6 if first else 9,
            [
                pltpu.VMEM((rows + (INFO if first else 0), ranks * 2 * LANES), bf16),
                pltpu.VMEM((ranks * 2 * LANES, cap), bf16),
                pltpu.VMEM((rows, cap), bf16),
                pltpu.VMEM((count * bands * GB, LANES), f32),
                pltpu.VMEM((count * bands * GB, LANES), f32),
                pltpu.VMEM((count, bands * GB, 2 * LANES), bf16),
                pltpu.VMEM((count, bands, 2 * GB, LANES), bf16),
                pltpu.VMEM((tails, bands, 2 * GB, LANES), bf16),
                pltpu.VMEM((count, N, LANES), f32),
                pltpu.VMEM((tails, N, LANES), f32),
            ],
            flops=16 * 10**9,
            smem=(4, 5),
        )
        results = run(received, *tables, weight, core, *kept)
        if first:
            kept = list(results[2:])
        halves += halve(results[0], results[1], "band")
    return vmem_call(
        functools.partial(sum_kernel, planes, own_rows),
        jax.ShapeDtypeStruct((held, own_rows, N), f32),
        len(halves),
    )(*halves)


def solution(mesh):
    placed = (P("band", "fft"), P("band"), P("fft"), P("fft"), P())

    return jax.shard_map(
        shards, mesh=mesh, in_specs=placed, out_specs=P("fft", "band", None), check_vma=False
    )
```

```python
import functools
import math

import jax
import jax.numpy as jnp
import numpy as np
from jax import lax
from jax.experimental import pallas as pl
from jax.experimental.pallas import tpu as pltpu
from jax.sharding import PartitionSpec as P


N = 144
GB = 72
LANES = 128
TAIL = N - LANES
SHARE = LANES // TAIL
PAIRS = 12
INFO = 16
GROUPS = 3


def wave_tables():
    freqs = np.arange(GB) - GB // 2
    angles = (freqs[:, None] * np.arange(N)[None, :] % N) * (2.0 * math.pi / N)
    cosine, sine = np.cos(angles), np.sin(angles)
    rows = np.zeros((2 * LANES, 2 * LANES), np.float32)
    ends = np.zeros((SHARE, 2 * LANES, 2 * LANES), np.float32)
    for col, real_from, imag_from in ((0, cosine, -sine), (1, sine, cosine)):
        rows[:GB, col * LANES : (col + 1) * LANES] = real_from[:, :LANES]
        rows[LANES : LANES + GB, col * LANES : (col + 1) * LANES] = imag_from[:, :LANES]
        for j in range(SHARE):
            at = col * LANES + j * TAIL
            ends[j, :GB, at : at + TAIL] = real_from[:, LANES:]
            ends[j, LANES : LANES + GB, at : at + TAIL] = imag_from[:, LANES:]
    cols = np.block([[cosine.T, -sine.T], [sine.T, cosine.T]])
    ends = ends.reshape(SHARE * 2 * LANES, 2 * LANES)
    return [jnp.asarray(x, jnp.bfloat16) for x in (rows, ends, cols)]


def stick_constants(planes, ranks):
    freqs = np.arange(GB) - GB // 2
    angles = (np.arange(N)[:, None] * freqs[None, :] % N) * (2.0 * math.pi / N)
    cosine, sine = np.cos(angles), np.sin(angles)
    held = sum(planes)
    ordered = sum(ranks * up(2 * count, 8) for count in planes)
    fixed = np.zeros((2, N + ordered, up(max(2 * LANES, ranks * held), LANES)), np.float32)
    fixed[0, :N, : 2 * GB] = np.concatenate([cosine, -sine], axis=1)
    fixed[1, :N, : 2 * GB] = np.concatenate([sine, cosine], axis=1)
    row, base = N, 0
    for count in planes:
        for d in range(ranks):
            for part in range(2):
                for j in range(count):
                    fixed[part, row + part * count + j, d * held + base + j] = 1
            row += up(2 * count, 8)
        base += count
    return jnp.asarray(fixed.reshape(-1, fixed.shape[2]), jnp.bfloat16)


def lane_group(rows, dtype):
    group = lax.broadcasted_iota(jnp.int32, (rows, LANES), 1) // 32
    return [(group == g).astype(jnp.float32).astype(dtype) for g in range(GROUPS + 1)]


def stick_kernel(planes, ranks, *refs):
    chunks = len(planes)
    outs, scratch = refs[5 : 5 + chunks], refs[5 + chunks :]
    count_here, slot_of, fixed, coef, column, done, low, high, ends = scratch[:9]
    mains, rests = scratch[9 : 9 + chunks], scratch[9 + chunks :]
    bands, slots = coef.shape[0], column.shape[0]
    inside = (count_here, slot_of, fixed, coef, column)
    copies = [
        pltpu.make_async_copy(src, to, done.at[i]) for i, (src, to) in enumerate(zip(refs, inside))
    ]
    for copy in copies:
        copy.start()
    for main, rest, count in zip(mains, rests, planes):
        if 2 * count * bands < main.shape[1]:
            main[...] = jnp.zeros_like(main)
            rest[...] = jnp.zeros_like(rest)

    def product(x, y, dims):
        return lax.dot_general(x, y, (dims, ((), ())), preferred_element_type=jnp.float32)

    copies[1].wait()
    copies[2].wait()
    held = slot_of[...].reshape(1, -1)
    at_pos = lax.broadcasted_iota(jnp.int32, (N, held.shape[1]), 0) == held
    at_pos = jnp.where(at_pos, 1.0, 0.0).astype(jnp.bfloat16)
    table = 0.0
    ordered = fixed.shape[0] // 2 - N
    for part in range(2):
        at = part * (N + ordered)
        pos = fixed[at : at + N]
        order = fixed[at + N : at + N + ordered, : held.shape[1]]
        rows_of_slot = product(at_pos, pos, ((0,), (0,))).astype(jnp.bfloat16)
        table = table + product(order, rows_of_slot, ((1,), (0,)))
    table = table.astype(jnp.bfloat16)

    stride = low.shape[0] // bands
    copies[3].wait()
    for s in range(slots):
        tile, shift = divmod(s * 2 * GB, LANES)
        x = coef[:, tile * LANES : (tile + 2) * LANES].astype(jnp.float32)
        if shift:
            x = pltpu.roll(x, 2 * LANES - shift, 1)
        low[pl.ds(s, bands, stride=stride), :] = x[:, :LANES]
        high[pl.ds(s, bands, stride=stride), :] = x[:, LANES:]

    for b in range(bands):
        here = slice(b * stride, b * stride + slots)
        x = jnp.concatenate([low[here], high[here]], axis=1).astype(jnp.bfloat16)
        x = jnp.concatenate([x[:LANES]] + [x[LANES:]] * 4, axis=0)
        val = product(table, x, ((1,), (1,)))
        at = 0
        for main, rest, count in zip(mains, rests, planes):
            for d in range(ranks):
                part = val[at : at + 2 * count]
                main[d, pl.ds(b, 2 * count, stride=bands), :] = part[:, :LANES]
                rest[d, pl.ds(b, 2 * count, stride=bands), :] = part[:, LANES:]
                at += up(2 * count, 8)

    copies[0].wait()
    copies[4].wait()
    c = column[...].reshape(1, -1).astype(jnp.float32)
    gx = jnp.floor((c + 0.5) * (1.0 / GB))
    row = lax.broadcasted_iota(jnp.int32, (INFO, slots), 0)
    live = count_here[0].astype(jnp.float32)
    info = jnp.where(
        row == 0, gx, jnp.where(row == 1, c - GB * gx, jnp.where(row == 2, live, 0.0))
    )
    ends[...] = jnp.zeros_like(ends)
    ends[:, : slots - LANES] = info[:, LANES:]
    tail_info = pltpu.roll(ends[...], 96, 1)

    for c, (out, main, rest) in enumerate(zip(outs, mains, rests)):
        rows = main.shape[1]
        span = rows // GROUPS
        masks = lane_group(span, jnp.float32)
        at = rows + (INFO if c == 0 else 0)
        for d in range(ranks):
            out[d, :rows, :] = main[d].astype(jnp.bfloat16)
            packed = rest[d, :span, :] * masks[0]
            for g in range(1, GROUPS):
                packed = packed + rest[d, g * span : (g + 1) * span, :] * masks[g]
            if c == 0:
                out[d, rows:at, :] = info[:, :LANES].astype(jnp.bfloat16)
                packed = packed + jnp.concatenate(
                    [tail_info, jnp.zeros((span - INFO, LANES), jnp.float32)], axis=0
                )
            out[d, at:, :] = packed.astype(jnp.bfloat16)


def plane_kernel(first, bands, ranks, planes, span, owners, own_rows, *refs):
    if first:
        recv, row_tab, end_tab, col_tab, weight, core, keep, send, turn, gx_of, gy_hot = refs[:11]
    else:
        recv, row_tab, end_tab, col_tab, weight, core, turn, gx_of, gy_hot, keep, send = refs[:11]
    lhs, pick, sticks, real, imag, both, half, tail, acc, acc_tail = refs[11:]
    rows = GROUPS * span
    total = rows + INFO if first else rows
    live = planes * bands
    cap = turn.shape[1]

    if first:
        place = lax.broadcasted_iota(jnp.int32, (1, cap), 1).astype(jnp.float32)
        start = jnp.zeros((1, 1), jnp.float32)
        for src in range(ranks):
            count = recv[src, rows : rows + INFO, :].astype(jnp.float32)[2:3, 0:1]
            t = place - start
            turn[src : src + 1, :] = jnp.where(jnp.logical_and(t >= 0, t < count), t, -1.0)
            start = start + count

    masks = lane_group(span, jnp.bfloat16)
    k = lax.broadcasted_iota(jnp.int32, (2 * LANES, cap), 0)
    slot = jnp.where(k < LANES, k, LANES + k % 32).astype(jnp.float32)
    for src in range(ranks):
        at = src * 2 * LANES
        pick[at : at + 2 * LANES, :] = jnp.where(slot == turn[src : src + 1, :], 1.0, 0.0).astype(
            jnp.bfloat16
        )
        packed = recv[src, total : total + span, :]
        pieces = [packed * masks[g] for g in range(GROUPS)]
        if first:
            pieces.append((packed * masks[GROUPS])[:INFO])
        lhs[:, at : at + LANES] = recv[src, :total, :]
        lhs[:, at + LANES : at + 2 * LANES] = jnp.concatenate(pieces, axis=0)
    compact = jnp.dot(lhs[...], pick[...], preferred_element_type=jnp.float32)
    sticks[...] = compact[:rows].astype(jnp.bfloat16)

    if first:
        info = jnp.concatenate(
            [compact[rows:], jnp.zeros((LANES - INFO, cap), jnp.float32)], axis=0
        ).T
        lane = lax.broadcasted_iota(jnp.int32, (cap, LANES), 1).astype(jnp.float32)
        gx_of[...] = jnp.broadcast_to(info[:, 0:1], (cap, LANES)).astype(jnp.bfloat16)
        gy_hot[...] = jnp.where(info[:, 1:2] == lane, 1.0, 0.0).astype(jnp.bfloat16)

    def put(step, carry):
        for u in range(PAIRS):
            pair = PAIRS * step + u
            hot = []
            for side in range(2):
                gx = (2 * pair + side).astype(jnp.float32).astype(jnp.bfloat16)
                hot.append(jnp.where(gx_of[...] == gx, gy_hot[...], jnp.zeros((), jnp.bfloat16)))
            placed = jnp.dot(
                sticks[...], jnp.concatenate(hot, axis=1), preferred_element_type=jnp.float32
            )
            for side in range(2):
                lanes = slice(side * LANES, (side + 1) * LANES)
                at = 2 * pair + side
                real[pl.ds(at, live, stride=GB), :] = placed[:live, lanes]
                imag[pl.ds(at, live, stride=GB), :] = placed[live : 2 * live, lanes]
        return carry

    lax.fori_loop(0, GB // 2 // PAIRS, put, 0)

    acc[...] = jnp.zeros_like(acc)
    acc_tail[...] = jnp.zeros_like(acc_tail)

    def stacked(piece):
        return jnp.concatenate([piece[:, :LANES], piece[:, LANES:]], axis=0).astype(jnp.bfloat16)

    def rows_of(step, carry):
        for u in range(deep):
            j = step * deep + u
            at = pl.ds(pl.multiple_of(j * (bands * GB), 8), bands * GB)
            x = jnp.concatenate(
                [real[at, :].astype(jnp.bfloat16), imag[at, :].astype(jnp.bfloat16)], axis=1
            )
            both[j] = x
            h = jnp.dot(x, row_tab[...], preferred_element_type=jnp.float32)
            for b in range(bands):
                half[j, b] = stacked(h[b * GB : (b + 1) * GB])
        return carry

    deep = largest(planes, 3)
    lax.fori_loop(0, planes // deep, rows_of, 0)

    tails = tail.shape[0]
    for t in range(tails):
        js = range(t * SHARE, min(planes, (t + 1) * SHARE))
        x = jnp.concatenate([both[j] for j in js], axis=1)
        h = jnp.dot(x, end_tab[: len(js) * 2 * LANES, :], preferred_element_type=jnp.float32)
        for b in range(bands):
            tail[t, b] = stacked(h[b * GB : (b + 1) * GB])

    wide = largest(bands, 4)

    def columns_of(step, carry):
        pieces = []
        for u in range(wide):
            b = wide * step + u
            pieces += [(acc, j, half, b) for j in range(planes)]
        for t in range(tails):
            pieces += [(acc_tail, t, tail, wide * step + u) for u in range(wide)]
        for i in range(0, len(pieces), 2):
            two = pieces[i : i + 2]
            x = jnp.concatenate([src[j, b] for _, j, src, b in two], axis=1)
            wave = jnp.dot(col_tab[...], x, preferred_element_type=jnp.float32)
            re, im = wave[:N], wave[N:]
            sq = re * re + im * im
            for side, (to, j, _, b) in enumerate(two):
                to[j] = to[j] + sq[:, side * LANES : (side + 1) * LANES] * weight[b]
        return carry

    lax.fori_loop(0, bands // wide, columns_of, 0)

    def deal(mine_bit):
        for o in range(owners):
            to = keep if o % 2 == mine_bit else send
            mine = slice(o * own_rows, (o + 1) * own_rows)
            for j in range(planes):
                to[o // 2, j, :own_rows, :] = acc[j, mine, :].astype(jnp.bfloat16)
            for t in range(tails):
                to[o // 2, planes + t, :own_rows, :] = acc_tail[t, mine, :].astype(jnp.bfloat16)

    @pl.when(core[0] == 0)
    def _():
        deal(0)

    @pl.when(core[0] != 0)
    def _():
        deal(1)


def sum_kernel(planes, own_rows, *refs):
    *parts, out = refs
    base = 0
    for c, count in enumerate(planes):
        total = parts[2 * c][...].astype(jnp.float32) + parts[2 * c + 1][...].astype(jnp.float32)
        for j in range(count):
            at = j % SHARE * TAIL
            out[base + j, :, :LANES] = total[j, :own_rows]
            out[base + j, :, LANES:] = total[count + j // SHARE, :own_rows, at : at + TAIL]
        base += count


def up(n, m):
    return -(-n // m) * m


def largest(n, most):
    return max(d for d in range(1, most + 1) if n % d == 0)


def vmem_call(kernel, out_shape, n_in, scratch=(), flops=1, smem=(), far=()):
    vmem_scratch = [m for m in scratch if m.memory_space == pltpu.VMEM]
    used = sum(math.prod(m.shape) * jnp.dtype(m.dtype).itemsize for m in vmem_scratch)
    vmem = pl.BlockSpec(memory_space=pltpu.VMEM)
    scalar = pl.BlockSpec(memory_space=pltpu.SMEM)
    hbm = pl.BlockSpec(memory_space=pltpu.HBM)
    many = isinstance(out_shape, list)
    return pl.pallas_call(
        kernel,
        out_shape=out_shape,
        in_specs=[scalar if i in smem else hbm if i in far else vmem for i in range(n_in)],
        out_specs=[vmem] * len(out_shape) if many else vmem,
        scratch_shapes=list(scratch),
        compiler_params=pltpu.CompilerParams(vmem_limit_bytes=62 * 2**20 if far else min(62 * 2**20, used + 12 * 2**20)),
        cost_estimate=pl.CostEstimate(flops=flops, bytes_accessed=1 << 20, transcendentals=0),
    )


def partners(axis, bit):
    return [(i, i ^ (1 << bit)) for i in range(lax.axis_size(axis))]


def halve(keep, send, axis):
    bit = 0
    while True:
        got = lax.ppermute(send, axis, partners(axis, bit))
        if keep.shape[0] == 1:
            return keep[0], got[0]
        whole = (keep.astype(jnp.float32) + got.astype(jnp.float32)).astype(keep.dtype)
        bit += 1
        here = lax.axis_index(axis) >> bit & 1
        pairs = whole.reshape((whole.shape[0] // 2, 2) + whole.shape[1:])
        keep = lax.dynamic_index_in_dim(pairs, here, 1, keepdims=False)
        send = lax.dynamic_index_in_dim(pairs, 1 - here, 1, keepdims=False)


def shards(coefficients, occupations, columns, counts, plane_slot):
    bands = coefficients.shape[0]
    ranks = lax.axis_size("fft")
    owners = lax.axis_size("band")
    slots = columns.shape[0]
    held = plane_slot.shape[0] // ranks
    last = min(SHARE, held // 2)
    planes = (held - last, last)
    cap = up(ranks * slots * 2 // 5, LANES)
    own_rows = N // owners
    bf16, f32 = jnp.bfloat16, jnp.float32

    weight = occupations / (bands * owners)
    core = (lax.axis_index("band") & 1)[None]
    tables = wave_tables()

    spans = [up(-(-2 * count * bands // GROUPS), 16) for count in planes]
    fixed = stick_constants(planes, ranks)
    stride = up(slots, 8) + 8
    outgoing = vmem_call(
        functools.partial(stick_kernel, planes, ranks),
        [
            jax.ShapeDtypeStruct((ranks, 4 * span + (INFO if c == 0 else 0), LANES), bf16)
            for c, span in enumerate(spans)
        ],
        5,
        [
            pltpu.SMEM(counts.shape, jnp.int32),
            pltpu.VMEM(plane_slot.shape, jnp.int32),
            pltpu.VMEM(fixed.shape, bf16),
            pltpu.VMEM(coefficients.shape, bf16),
            pltpu.VMEM(columns.shape, jnp.int32),
            pltpu.SemaphoreType.DMA((5,)),
        ]
        + [pltpu.VMEM((bands * stride, LANES), f32)] * 2
        + [pltpu.VMEM((INFO, LANES), f32)]
        + [pltpu.VMEM((ranks, GROUPS * span, LANES), f32) for span in spans * 2],
        flops=4 * 10**9,
        far=range(5),
    )(counts, plane_slot, fixed, coefficients, columns)
    kept_shapes = [
        jax.ShapeDtypeStruct((ranks, cap), f32),
        jax.ShapeDtypeStruct((cap, LANES), bf16),
        jax.ShapeDtypeStruct((cap, LANES), bf16),
    ]
    kept, halves = [], []
    for c, (count, span) in enumerate(zip(planes, spans)):
        first = c == 0
        received = lax.all_to_all(outgoing[c], "fft", split_axis=0, concat_axis=0, tiled=True)
        rows = GROUPS * span
        tails = -(-count // SHARE)
        dens_shape = jax.ShapeDtypeStruct(
            (owners // 2, count + tails, up(own_rows, 8), LANES), bf16
        )
        run = vmem_call(
            functools.partial(plane_kernel, first, bands, ranks, count, span, owners, own_rows),
            [dens_shape] * 2 + (kept_shapes if first else []),
            6 if first else 9,
            [
                pltpu.VMEM((rows + (INFO if first else 0), ranks * 2 * LANES), bf16),
                pltpu.VMEM((ranks * 2 * LANES, cap), bf16),
                pltpu.VMEM((rows, cap), bf16),
                pltpu.VMEM((count * bands * GB, LANES), f32),
                pltpu.VMEM((count * bands * GB, LANES), f32),
                pltpu.VMEM((count, bands * GB, 2 * LANES), bf16),
                pltpu.VMEM((count, bands, 2 * GB, LANES), bf16),
                pltpu.VMEM((tails, bands, 2 * GB, LANES), bf16),
                pltpu.VMEM((count, N, LANES), f32),
                pltpu.VMEM((tails, N, LANES), f32),
            ],
            flops=16 * 10**9,
            smem=(4, 5),
        )
        results = run(received, *tables, weight, core, *kept)
        if first:
            kept = list(results[2:])
        halves += halve(results[0], results[1], "band")
    return vmem_call(
        functools.partial(sum_kernel, planes, own_rows),
        jax.ShapeDtypeStruct((held, own_rows, N), f32),
        len(halves),
    )(*halves)


def solution(mesh):
    placed = (P("band", "fft"), P("band"), P("fft"), P("fft"), P())

    return jax.shard_map(
        shards, mesh=mesh, in_specs=placed, out_specs=P("fft", "band", None), check_vma=False
    )
```

```python
import functools
import math

import jax
import jax.numpy as jnp
import numpy as np
from jax import lax
from jax.experimental import pallas as pl
from jax.experimental.pallas import tpu as pltpu
from jax.sharding import PartitionSpec as P


N = 144
GB = 72
LANES = 128
TAIL = N - LANES
SHARE = LANES // TAIL
PAIRS = 12
INFO = 16
GROUPS = 3


def wave_tables():
    freqs = np.arange(GB) - GB // 2
    angles = (freqs[:, None] * np.arange(N)[None, :] % N) * (2.0 * math.pi / N)
    cosine, sine = np.cos(angles), np.sin(angles)
    rows = np.zeros((2 * LANES, 2 * LANES), np.float32)
    ends = np.zeros((SHARE, 2 * LANES, 2 * LANES), np.float32)
    for col, real_from, imag_from in ((0, cosine, -sine), (1, sine, cosine)):
        rows[:GB, col * LANES : (col + 1) * LANES] = real_from[:, :LANES]
        rows[LANES : LANES + GB, col * LANES : (col + 1) * LANES] = imag_from[:, :LANES]
        for j in range(SHARE):
            at = col * LANES + j * TAIL
            ends[j, :GB, at : at + TAIL] = real_from[:, LANES:]
            ends[j, LANES : LANES + GB, at : at + TAIL] = imag_from[:, LANES:]
    cols = np.block([[cosine.T, -sine.T], [sine.T, cosine.T]])
    ends = ends.reshape(SHARE * 2 * LANES, 2 * LANES)
    return [jnp.asarray(x, jnp.bfloat16) for x in (rows, ends, cols)]


def stick_constants(planes, ranks):
    freqs = np.arange(GB) - GB // 2
    angles = (np.arange(N)[:, None] * freqs[None, :] % N) * (2.0 * math.pi / N)
    cosine, sine = np.cos(angles), np.sin(angles)
    held = sum(planes)
    ordered = sum(ranks * up(2 * count, 8) for count in planes)
    fixed = np.zeros((2, N + ordered, up(max(2 * LANES, ranks * held), LANES)), np.float32)
    fixed[0, :N, : 2 * GB] = np.concatenate([cosine, -sine], axis=1)
    fixed[1, :N, : 2 * GB] = np.concatenate([sine, cosine], axis=1)
    row, base = N, 0
    for count in planes:
        for d in range(ranks):
            for part in range(2):
                for j in range(count):
                    fixed[part, row + part * count + j, d * held + base + j] = 1
            row += up(2 * count, 8)
        base += count
    return jnp.asarray(fixed.reshape(-1, fixed.shape[2]), jnp.bfloat16)


def lane_group(rows, dtype):
    group = lax.broadcasted_iota(jnp.int32, (rows, LANES), 1) // 32
    return [(group == g).astype(jnp.float32).astype(dtype) for g in range(GROUPS + 1)]


def stick_kernel(planes, ranks, *refs):
    chunks = len(planes)
    outs, scratch = refs[5 : 6 + (chunks - 1) * ranks], refs[6 + (chunks - 1) * ranks :]
    me = lax.axis_index("fft")
    count_here, slot_of, fixed, coef, column, done, low, high, ends = scratch[:9]
    mains, rests = scratch[9 : 9 + chunks], scratch[9 + chunks :]
    bands, slots = coef.shape[0], column.shape[0]
    inside = (count_here, slot_of, fixed, coef, column)
    copies = [
        pltpu.make_async_copy(src, to, done.at[i]) for i, (src, to) in enumerate(zip(refs, inside))
    ]
    for copy in copies:
        copy.start()
    for main, rest, count in zip(mains, rests, planes):
        if 2 * count * bands < main.shape[1]:
            main[...] = jnp.zeros_like(main)
            rest[...] = jnp.zeros_like(rest)

    def product(x, y, dims):
        return lax.dot_general(x, y, (dims, ((), ())), preferred_element_type=jnp.float32)

    copies[1].wait()
    copies[2].wait()
    held = slot_of[...].reshape(1, -1)
    at_pos = lax.broadcasted_iota(jnp.int32, (N, held.shape[1]), 0) == held
    at_pos = jnp.where(at_pos, 1.0, 0.0).astype(jnp.bfloat16)
    table = 0.0
    ordered = fixed.shape[0] // 2 - N
    for part in range(2):
        at = part * (N + ordered)
        pos = fixed[at : at + N]
        order = fixed[at + N : at + N + ordered, : held.shape[1]]
        rows_of_slot = product(at_pos, pos, ((0,), (0,))).astype(jnp.bfloat16)
        table = table + product(order, rows_of_slot, ((1,), (0,)))
    table = table.astype(jnp.bfloat16)

    stride = low.shape[0] // bands
    copies[3].wait()
    for s in range(slots):
        tile, shift = divmod(s * 2 * GB, LANES)
        x = coef[:, tile * LANES : (tile + 2) * LANES].astype(jnp.float32)
        if shift:
            x = pltpu.roll(x, 2 * LANES - shift, 1)
        low[pl.ds(s, bands, stride=stride), :] = x[:, :LANES]
        high[pl.ds(s, bands, stride=stride), :] = x[:, LANES:]

    for b in range(bands):
        here = slice(b * stride, b * stride + slots)
        x = jnp.concatenate([low[here], high[here]], axis=1).astype(jnp.bfloat16)
        x = jnp.concatenate([x[:LANES]] + [x[LANES:]] * 4, axis=0)
        val = product(table, x, ((1,), (1,)))
        at = 0
        for main, rest, count in zip(mains, rests, planes):
            for d in range(ranks):
                part = val[at : at + 2 * count]
                main[d, pl.ds(b, 2 * count, stride=bands), :] = part[:, :LANES]
                rest[d, pl.ds(b, 2 * count, stride=bands), :] = part[:, LANES:]
                at += up(2 * count, 8)

    copies[0].wait()
    copies[4].wait()
    c = column[...].reshape(1, -1).astype(jnp.float32)
    gx = jnp.floor((c + 0.5) * (1.0 / GB))
    row = lax.broadcasted_iota(jnp.int32, (INFO, slots), 0)
    live = count_here[0].astype(jnp.float32)
    info = jnp.where(
        row == 0, gx, jnp.where(row == 1, c - GB * gx, jnp.where(row == 2, live, 0.0))
    )
    ends[...] = jnp.zeros_like(ends)
    ends[:, : slots - LANES] = info[:, LANES:]
    tail_info = pltpu.roll(ends[...], 96, 1)

    for c, (main, rest) in enumerate(zip(mains, rests)):
        rows = main.shape[1]
        span = rows // GROUPS
        masks = lane_group(span, jnp.float32)
        at = rows + (INFO if c == 0 else 0)
        for k in range(ranks):
            out, d = (outs[0].at[k], k) if c == 0 else (outs[1 + (c - 1) * ranks + k], me ^ k)
            out[:rows, :] = main[d].astype(jnp.bfloat16)
            packed = rest[d, :span, :] * masks[0]
            for g in range(1, GROUPS):
                packed = packed + rest[d, g * span : (g + 1) * span, :] * masks[g]
            if c == 0:
                out[rows:at, :] = info[:, :LANES].astype(jnp.bfloat16)
                packed = packed + jnp.concatenate(
                    [tail_info, jnp.zeros((span - INFO, LANES), jnp.float32)], axis=0
                )
            out[at:, :] = packed.astype(jnp.bfloat16)


def plane_kernel(first, bands, ranks, planes, span, owners, own_rows, *refs):
    if first:
        recv, row_tab, end_tab, col_tab, weight, core, keep, send, turn, gx_of, gy_hot = refs[:11]
        blocks, source = [recv.at[src] for src in range(ranks)], lambda k: slice(k, k + 1)
    else:
        blocks, refs = refs[:ranks], refs[ranks - 1 :]
        _, row_tab, end_tab, col_tab, weight, core, turn, gx_of, gy_hot, keep, send = refs[:11]
        me = lax.axis_index("fft")
        source = lambda k: pl.ds(me ^ k, 1)
    lhs, pick, sticks, real, imag, both, half, tail, acc, acc_tail = refs[11:]
    rows = GROUPS * span
    total = rows + INFO if first else rows
    live = planes * bands
    cap = turn.shape[1]

    if first:
        place = lax.broadcasted_iota(jnp.int32, (1, cap), 1).astype(jnp.float32)
        start = jnp.zeros((1, 1), jnp.float32)
        for src in range(ranks):
            count = blocks[src][rows : rows + INFO, :].astype(jnp.float32)[2:3, 0:1]
            t = place - start
            turn[src : src + 1, :] = jnp.where(jnp.logical_and(t >= 0, t < count), t, -1.0)
            start = start + count

    masks = lane_group(span, jnp.bfloat16)
    k = lax.broadcasted_iota(jnp.int32, (2 * LANES, cap), 0)
    slot = jnp.where(k < LANES, k, LANES + k % 32).astype(jnp.float32)
    for src in range(ranks):
        at = src * 2 * LANES
        pick[at : at + 2 * LANES, :] = jnp.where(slot == turn[source(src), :], 1.0, 0.0).astype(
            jnp.bfloat16
        )
        packed = blocks[src][total : total + span, :]
        pieces = [packed * masks[g] for g in range(GROUPS)]
        if first:
            pieces.append((packed * masks[GROUPS])[:INFO])
        lhs[:, at : at + LANES] = blocks[src][:total, :]
        lhs[:, at + LANES : at + 2 * LANES] = jnp.concatenate(pieces, axis=0)
    compact = jnp.dot(lhs[...], pick[...], preferred_element_type=jnp.float32)
    sticks[...] = compact[:rows].astype(jnp.bfloat16)

    if first:
        info = jnp.concatenate(
            [compact[rows:], jnp.zeros((LANES - INFO, cap), jnp.float32)], axis=0
        ).T
        lane = lax.broadcasted_iota(jnp.int32, (cap, LANES), 1).astype(jnp.float32)
        gx_of[...] = jnp.broadcast_to(info[:, 0:1], (cap, LANES)).astype(jnp.bfloat16)
        gy_hot[...] = jnp.where(info[:, 1:2] == lane, 1.0, 0.0).astype(jnp.bfloat16)

    def put(step, carry):
        for u in range(PAIRS):
            pair = PAIRS * step + u
            hot = []
            for side in range(2):
                gx = (2 * pair + side).astype(jnp.float32).astype(jnp.bfloat16)
                hot.append(jnp.where(gx_of[...] == gx, gy_hot[...], jnp.zeros((), jnp.bfloat16)))
            placed = jnp.dot(
                sticks[...], jnp.concatenate(hot, axis=1), preferred_element_type=jnp.float32
            )
            for side in range(2):
                lanes = slice(side * LANES, (side + 1) * LANES)
                at = 2 * pair + side
                real[pl.ds(at, live, stride=GB), :] = placed[:live, lanes]
                imag[pl.ds(at, live, stride=GB), :] = placed[live : 2 * live, lanes]
        return carry

    lax.fori_loop(0, GB // 2 // PAIRS, put, 0)

    acc[...] = jnp.zeros_like(acc)
    acc_tail[...] = jnp.zeros_like(acc_tail)

    def stacked(piece):
        return jnp.concatenate([piece[:, :LANES], piece[:, LANES:]], axis=0).astype(jnp.bfloat16)

    def rows_of(step, carry):
        for u in range(deep):
            j = step * deep + u
            at = pl.ds(pl.multiple_of(j * (bands * GB), 8), bands * GB)
            x = jnp.concatenate(
                [real[at, :].astype(jnp.bfloat16), imag[at, :].astype(jnp.bfloat16)], axis=1
            )
            both[j] = x
            h = jnp.dot(x, row_tab[...], preferred_element_type=jnp.float32)
            for b in range(bands):
                half[j, b] = stacked(h[b * GB : (b + 1) * GB])
        return carry

    deep = largest(planes, 3)
    lax.fori_loop(0, planes // deep, rows_of, 0)

    tails = tail.shape[0]
    for t in range(tails):
        js = range(t * SHARE, min(planes, (t + 1) * SHARE))
        x = jnp.concatenate([both[j] for j in js], axis=1)
        h = jnp.dot(x, end_tab[: len(js) * 2 * LANES, :], preferred_element_type=jnp.float32)
        for b in range(bands):
            tail[t, b] = stacked(h[b * GB : (b + 1) * GB])

    wide = largest(bands, 4)

    def columns_of(step, carry):
        pieces = []
        for u in range(wide):
            b = wide * step + u
            pieces += [(acc, j, half, b) for j in range(planes)]
        for t in range(tails):
            pieces += [(acc_tail, t, tail, wide * step + u) for u in range(wide)]
        for i in range(0, len(pieces), 2):
            two = pieces[i : i + 2]
            x = jnp.concatenate([src[j, b] for _, j, src, b in two], axis=1)
            wave = jnp.dot(col_tab[...], x, preferred_element_type=jnp.float32)
            re, im = wave[:N], wave[N:]
            sq = re * re + im * im
            for side, (to, j, _, b) in enumerate(two):
                to[j] = to[j] + sq[:, side * LANES : (side + 1) * LANES] * weight[b]
        return carry

    lax.fori_loop(0, bands // wide, columns_of, 0)

    def deal(mine_bit):
        for o in range(owners):
            to = keep if o % 2 == mine_bit else send
            mine = slice(o * own_rows, (o + 1) * own_rows)
            for j in range(planes):
                to[o // 2, j, :own_rows, :] = acc[j, mine, :].astype(jnp.bfloat16)
            for t in range(tails):
                to[o // 2, planes + t, :own_rows, :] = acc_tail[t, mine, :].astype(jnp.bfloat16)

    @pl.when(core[0] == 0)
    def _():
        deal(0)

    @pl.when(core[0] != 0)
    def _():
        deal(1)


def sum_kernel(planes, own_rows, *refs):
    *parts, out = refs
    base = 0
    for c, count in enumerate(planes):
        total = parts[2 * c][...].astype(jnp.float32) + parts[2 * c + 1][...].astype(jnp.float32)
        for j in range(count):
            at = j % SHARE * TAIL
            out[base + j, :, :LANES] = total[j, :own_rows]
            out[base + j, :, LANES:] = total[count + j // SHARE, :own_rows, at : at + TAIL]
        base += count


def up(n, m):
    return -(-n // m) * m


def largest(n, most):
    return max(d for d in range(1, most + 1) if n % d == 0)


def vmem_call(kernel, out_shape, n_in, scratch=(), flops=1, smem=(), far=()):
    vmem_scratch = [m for m in scratch if m.memory_space == pltpu.VMEM]
    used = sum(math.prod(m.shape) * jnp.dtype(m.dtype).itemsize for m in vmem_scratch)
    vmem = pl.BlockSpec(memory_space=pltpu.VMEM)
    scalar = pl.BlockSpec(memory_space=pltpu.SMEM)
    hbm = pl.BlockSpec(memory_space=pltpu.HBM)
    many = isinstance(out_shape, list)
    return pl.pallas_call(
        kernel,
        out_shape=out_shape,
        in_specs=[scalar if i in smem else hbm if i in far else vmem for i in range(n_in)],
        out_specs=[vmem] * len(out_shape) if many else vmem,
        scratch_shapes=list(scratch),
        compiler_params=pltpu.CompilerParams(vmem_limit_bytes=62 * 2**20 if far else min(62 * 2**20, used + 12 * 2**20)),
        cost_estimate=pl.CostEstimate(flops=flops, bytes_accessed=1 << 20, transcendentals=0),
    )


def partners(axis, bit):
    return [(i, i ^ (1 << bit)) for i in range(lax.axis_size(axis))]


def halve(keep, send, axis):
    bit = 0
    while True:
        got = lax.ppermute(send, axis, partners(axis, bit))
        if keep.shape[0] == 1:
            return keep[0], got[0]
        whole = (keep.astype(jnp.float32) + got.astype(jnp.float32)).astype(keep.dtype)
        bit += 1
        here = lax.axis_index(axis) >> bit & 1
        pairs = whole.reshape((whole.shape[0] // 2, 2) + whole.shape[1:])
        keep = lax.dynamic_index_in_dim(pairs, here, 1, keepdims=False)
        send = lax.dynamic_index_in_dim(pairs, 1 - here, 1, keepdims=False)


def shards(coefficients, occupations, columns, counts, plane_slot):
    bands = coefficients.shape[0]
    ranks = lax.axis_size("fft")
    owners = lax.axis_size("band")
    slots = columns.shape[0]
    held = plane_slot.shape[0] // ranks
    last = min(SHARE, held // 2)
    planes = (held - last, last)
    cap = up(ranks * slots * 2 // 5, LANES)
    own_rows = N // owners
    bf16, f32 = jnp.bfloat16, jnp.float32

    weight = occupations / (bands * owners)
    core = (lax.axis_index("band") & 1)[None]
    tables = wave_tables()

    spans = [up(-(-2 * count * bands // GROUPS), 16) for count in planes]
    fixed = stick_constants(planes, ranks)
    stride = up(slots, 8) + 8
    outgoing = vmem_call(
        functools.partial(stick_kernel, planes, ranks),
        [jax.ShapeDtypeStruct((ranks, 4 * spans[0] + INFO, LANES), bf16)]
        + [jax.ShapeDtypeStruct((4 * spans[1], LANES), bf16)] * ranks,
        5,
        [
            pltpu.SMEM(counts.shape, jnp.int32),
            pltpu.VMEM(plane_slot.shape, jnp.int32),
            pltpu.VMEM(fixed.shape, bf16),
            pltpu.VMEM(coefficients.shape, bf16),
            pltpu.VMEM(columns.shape, jnp.int32),
            pltpu.SemaphoreType.DMA((5,)),
        ]
        + [pltpu.VMEM((bands * stride, LANES), f32)] * 2
        + [pltpu.VMEM((INFO, LANES), f32)]
        + [pltpu.VMEM((ranks, GROUPS * span, LANES), f32) for span in spans * 2],
        flops=4 * 10**9,
        far=range(5),
    )(counts, plane_slot, fixed, coefficients, columns)
    kept_shapes = [
        jax.ShapeDtypeStruct((ranks, cap), f32),
        jax.ShapeDtypeStruct((cap, LANES), bf16),
        jax.ShapeDtypeStruct((cap, LANES), bf16),
    ]
    kept, halves = [], []
    for c, (count, span) in enumerate(zip(planes, spans)):
        first = c == 0
        if first:
            received = [lax.all_to_all(outgoing[0], "fft", split_axis=0, concat_axis=0, tiled=True)]
        else:
            received = [outgoing[1]]
            for k in range(1, ranks):
                pairs = [(i, i ^ k) for i in range(ranks)]
                received.append(lax.ppermute(outgoing[1 + k], "fft", pairs))
        rows = GROUPS * span
        tails = -(-count // SHARE)
        dens_shape = jax.ShapeDtypeStruct(
            (owners // 2, count + tails, up(own_rows, 8), LANES), bf16
        )
        run = vmem_call(
            functools.partial(plane_kernel, first, bands, ranks, count, span, owners, own_rows),
            [dens_shape] * 2 + (kept_shapes if first else []),
            len(received) + (5 if first else 8),
            [
                pltpu.VMEM((rows + (INFO if first else 0), ranks * 2 * LANES), bf16),
                pltpu.VMEM((ranks * 2 * LANES, cap), bf16),
                pltpu.VMEM((rows, cap), bf16),
                pltpu.VMEM((count * bands * GB, LANES), f32),
                pltpu.VMEM((count * bands * GB, LANES), f32),
                pltpu.VMEM((count, bands * GB, 2 * LANES), bf16),
                pltpu.VMEM((count, bands, 2 * GB, LANES), bf16),
                pltpu.VMEM((tails, bands, 2 * GB, LANES), bf16),
                pltpu.VMEM((count, N, LANES), f32),
                pltpu.VMEM((tails, N, LANES), f32),
            ],
            flops=16 * 10**9,
            smem=(len(received) + 3, len(received) + 4),
        )
        results = run(*received, *tables, weight, core, *kept)
        if first:
            kept = list(results[2:])
        halves += halve(results[0], results[1], "band")
    return vmem_call(
        functools.partial(sum_kernel, planes, own_rows),
        jax.ShapeDtypeStruct((held, own_rows, N), f32),
        len(halves),
    )(*halves)


def solution(mesh):
    placed = (P("band", "fft"), P("band"), P("fft"), P("fft"), P())

    return jax.shard_map(
        shards, mesh=mesh, in_specs=placed, out_specs=P("fft", "band", None), check_vma=False
    )
```

```python
import functools
import math

import jax
import jax.numpy as jnp
import numpy as np
from jax import lax
from jax.experimental import pallas as pl
from jax.experimental.pallas import tpu as pltpu
from jax.sharding import PartitionSpec as P


N = 144
GB = 72
LANES = 128
TAIL = N - LANES
SHARE = LANES // TAIL
PAIRS = 12
INFO = 8
GROUPS = 4


def wave_tables():
    freqs = np.arange(GB) - GB // 2
    angles = (freqs[:, None] * np.arange(N)[None, :] % N) * (2.0 * math.pi / N)
    cosine, sine = np.cos(angles), np.sin(angles)
    rows = np.zeros((2 * LANES, 2 * LANES), np.float32)
    ends = np.zeros((SHARE, 2 * LANES, 2 * LANES), np.float32)
    for col, real_from, imag_from in ((0, cosine, -sine), (1, sine, cosine)):
        rows[:GB, col * LANES : (col + 1) * LANES] = real_from[:, :LANES]
        rows[LANES : LANES + GB, col * LANES : (col + 1) * LANES] = imag_from[:, :LANES]
        for j in range(SHARE):
            at = col * LANES + j * TAIL
            ends[j, :GB, at : at + TAIL] = real_from[:, LANES:]
            ends[j, LANES : LANES + GB, at : at + TAIL] = imag_from[:, LANES:]
    cols = np.block([[cosine.T, -sine.T], [sine.T, cosine.T]])
    ends = ends.reshape(SHARE * 2 * LANES, 2 * LANES)
    return [jnp.asarray(x, jnp.bfloat16) for x in (rows, ends, cols)]


def stick_constants(planes, ranks):
    freqs = np.arange(GB) - GB // 2
    angles = (np.arange(N)[:, None] * freqs[None, :] % N) * (2.0 * math.pi / N)
    cosine, sine = np.cos(angles), np.sin(angles)
    held = sum(planes)
    ordered = sum(ranks * up(2 * count, 8) for count in planes)
    fixed = np.zeros((2, N + ordered, up(max(2 * LANES, ranks * held), LANES)), np.float32)
    fixed[0, :N, : 2 * GB] = np.concatenate([cosine, -sine], axis=1)
    fixed[1, :N, : 2 * GB] = np.concatenate([sine, cosine], axis=1)
    row, base = N, 0
    for count in planes:
        for d in range(ranks):
            for part in range(2):
                for j in range(count):
                    fixed[part, row + part * count + j, d * held + base + j] = 1
            row += up(2 * count, 8)
        base += count
    return jnp.asarray(fixed.reshape(-1, fixed.shape[2]), jnp.bfloat16)


def lane_group(rows, dtype):
    group = lax.broadcasted_iota(jnp.int32, (rows, LANES), 1) // 32
    return [(group == g).astype(jnp.float32).astype(dtype) for g in range(GROUPS)]


def stick_kernel(planes, ranks, *refs):
    chunks = len(planes)
    outs, scratch = refs[5 : 6 + (chunks - 1) * ranks], refs[6 + (chunks - 1) * ranks :]
    me = lax.axis_index("fft")
    count_here, slot_of, fixed, coef, column, done, low, high, ends = scratch[:9]
    mains, rests = scratch[9 : 9 + chunks], scratch[9 + chunks :]
    bands, slots = coef.shape[0], column.shape[0]
    inside = (count_here, slot_of, fixed, coef, column)
    copies = [
        pltpu.make_async_copy(src, to, done.at[i]) for i, (src, to) in enumerate(zip(refs, inside))
    ]
    for copy in copies:
        copy.start()
    for main, rest, count in zip(mains, rests, planes):
        if 2 * count * bands < main.shape[1]:
            main[...] = jnp.zeros_like(main)
            rest[...] = jnp.zeros_like(rest)

    def product(x, y, dims):
        return lax.dot_general(x, y, (dims, ((), ())), preferred_element_type=jnp.float32)

    copies[1].wait()
    copies[2].wait()
    held = slot_of[...].reshape(1, -1)
    at_pos = lax.broadcasted_iota(jnp.int32, (N, held.shape[1]), 0) == held
    at_pos = jnp.where(at_pos, 1.0, 0.0).astype(jnp.bfloat16)
    table = 0.0
    ordered = fixed.shape[0] // 2 - N
    for part in range(2):
        at = part * (N + ordered)
        pos = fixed[at : at + N]
        order = fixed[at + N : at + N + ordered, : held.shape[1]]
        rows_of_slot = product(at_pos, pos, ((0,), (0,))).astype(jnp.bfloat16)
        table = table + product(order, rows_of_slot, ((1,), (0,)))
    table = table.astype(jnp.bfloat16)

    stride = low.shape[0] // bands
    copies[3].wait()
    for s in range(slots):
        tile, shift = divmod(s * 2 * GB, LANES)
        x = coef[:, tile * LANES : (tile + 2) * LANES].astype(jnp.float32)
        if shift:
            x = pltpu.roll(x, 2 * LANES - shift, 1)
        low[pl.ds(s, bands, stride=stride), :] = x[:, :LANES]
        high[pl.ds(s, bands, stride=stride), :] = x[:, LANES:]

    for b in range(bands):
        here = slice(b * stride, b * stride + slots)
        x = jnp.concatenate([low[here], high[here]], axis=1).astype(jnp.bfloat16)
        x = jnp.concatenate([x[:LANES]] + [x[LANES:]] * 4, axis=0)
        val = product(table, x, ((1,), (1,)))
        at = 0
        for main, rest, count in zip(mains, rests, planes):
            for d in range(ranks):
                part = val[at : at + 2 * count]
                main[d, pl.ds(b, 2 * count, stride=bands), :] = part[:, :LANES]
                rest[d, pl.ds(b, 2 * count, stride=bands), :] = part[:, LANES:]
                at += up(2 * count, 8)

    copies[0].wait()
    copies[4].wait()
    c = column[...].reshape(1, -1).astype(jnp.float32)
    gx = jnp.floor((c + 0.5) * (1.0 / GB))
    row = lax.broadcasted_iota(jnp.int32, (INFO, slots), 0)
    live = count_here[0].astype(jnp.float32)
    info = jnp.where(row % 3 == 0, gx, jnp.where(row % 3 == 1, c - GB * gx, live))
    ends[...] = jnp.zeros_like(ends)
    ends[:, : slots - LANES] = info[:, LANES:]
    row = lax.broadcasted_iota(jnp.int32, (INFO, LANES), 0)
    info = jnp.where(row < 3, info[:, :LANES], jnp.where(row < 5, ends[...], 0.0))

    for c, (main, rest, count) in enumerate(zip(mains, rests, planes)):
        rows = 2 * count * bands
        span = main.shape[1] // GROUPS
        masks = lane_group(span, jnp.float32)
        at = rows + (INFO if c == 0 else 0)
        for k in range(ranks):
            out, d = (outs[0].at[k], k) if c == 0 else (outs[1 + (c - 1) * ranks + k], me ^ k)
            out[:rows, :] = main[d, :rows, :].astype(jnp.bfloat16)
            packed = rest[d, :span, :] * masks[0]
            for g in range(1, GROUPS):
                packed = packed + rest[d, g * span : (g + 1) * span, :] * masks[g]
            if c == 0:
                out[rows:at, :] = info.astype(jnp.bfloat16)
            out[at:, :] = packed.astype(jnp.bfloat16)


def plane_kernel(first, bands, ranks, planes, span, owners, own_rows, *refs):
    if first:
        recv, row_tab, end_tab, col_tab, weight, core, keep, send, turn, gx_of, gy_hot = refs[:11]
        blocks, source = [recv.at[src] for src in range(ranks)], lambda k: slice(k, k + 1)
    else:
        blocks, refs = refs[:ranks], refs[ranks - 1 :]
        _, row_tab, end_tab, col_tab, weight, core, turn, gx_of, gy_hot, keep, send = refs[:11]
        me = lax.axis_index("fft")
        source = lambda k: pl.ds(me ^ k, 1)
    lhs, pick, sticks, real, imag, both, half, tail, acc, acc_tail = refs[11:]
    live = planes * bands
    rows = 2 * live
    total = rows + INFO if first else rows
    cap = turn.shape[1]

    if first:
        place = lax.broadcasted_iota(jnp.int32, (1, cap), 1).astype(jnp.float32)
        start = jnp.zeros((1, 1), jnp.float32)
        for src in range(ranks):
            count = blocks[src][rows : rows + INFO, :].astype(jnp.float32)[2:3, 0:1]
            t = place - start
            turn[src : src + 1, :] = jnp.where(jnp.logical_and(t >= 0, t < count), t, -1.0)
            start = start + count

    masks = lane_group(span, jnp.bfloat16)
    k = lax.broadcasted_iota(jnp.int32, (2 * LANES, cap), 0)
    slot = jnp.where(k < LANES, k, LANES + k % 32).astype(jnp.float32).astype(jnp.bfloat16)
    one, zero = jnp.ones((), jnp.bfloat16), jnp.zeros((), jnp.bfloat16)
    if first:
        info_row = lax.broadcasted_iota(jnp.int32, (INFO, LANES), 0)
        info_main = (info_row < 3).astype(jnp.float32).astype(jnp.bfloat16)
    for src in range(ranks):
        at = src * 2 * LANES
        wanted = jnp.broadcast_to(turn[source(src), :].astype(jnp.bfloat16), slot.shape)
        pick[at : at + 2 * LANES, :] = jnp.where(slot == wanted, one, zero)
        block, low, high = blocks[src], slice(at, at + LANES), slice(at + LANES, at + 2 * LANES)
        lhs[:rows, low] = block[:rows, :]
        packed = block[total : total + span, :]
        for g in range(GROUPS):
            here = slice(g * span, min(rows, (g + 1) * span))
            if here.start < here.stop:
                lhs[here, high] = (packed * masks[g])[: here.stop - here.start]
        if first:
            info = block[rows:total, :]
            lhs[rows:, low] = info * info_main
            lhs[rows:, high] = info * (one - info_main)
    compact = jnp.dot(lhs[...], pick[...], preferred_element_type=jnp.float32)
    sticks[...] = compact[:rows].astype(jnp.bfloat16)

    if first:
        info = jnp.concatenate(
            [compact[rows:], jnp.zeros((LANES - INFO, cap), jnp.float32)], axis=0
        ).T
        lane = lax.broadcasted_iota(jnp.int32, (cap, LANES), 1).astype(jnp.float32)
        gx, gy = (info[:, i : i + 1] + info[:, i + 3 : i + 4] for i in range(2))
        gx_of[...] = jnp.broadcast_to(gx, (cap, LANES)).astype(jnp.bfloat16)
        gy_hot[...] = jnp.where(gy == lane, 1.0, 0.0).astype(jnp.bfloat16)

    def put(step, carry):
        for u in range(PAIRS):
            pair = PAIRS * step + u
            hot = []
            for side in range(2):
                gx = (2 * pair + side).astype(jnp.float32).astype(jnp.bfloat16)
                hot.append(jnp.where(gx_of[...] == gx, gy_hot[...], jnp.zeros((), jnp.bfloat16)))
            placed = jnp.dot(
                sticks[...], jnp.concatenate(hot, axis=1), preferred_element_type=jnp.float32
            )
            for side in range(2):
                lanes = slice(side * LANES, (side + 1) * LANES)
                at = 2 * pair + side
                real[pl.ds(at, live, stride=GB), :] = placed[:live, lanes]
                imag[pl.ds(at, live, stride=GB), :] = placed[live : 2 * live, lanes]
        return carry

    lax.fori_loop(0, GB // 2 // PAIRS, put, 0)

    acc[...] = jnp.zeros_like(acc)
    acc_tail[...] = jnp.zeros_like(acc_tail)

    def stacked(piece):
        return jnp.concatenate([piece[:, :LANES], piece[:, LANES:]], axis=0).astype(jnp.bfloat16)

    def rows_of(step, carry):
        for u in range(deep):
            j = step * deep + u
            at = pl.ds(pl.multiple_of(j * (bands * GB), 8), bands * GB)
            x = jnp.concatenate(
                [real[at, :].astype(jnp.bfloat16), imag[at, :].astype(jnp.bfloat16)], axis=1
            )
            both[j] = x
            h = jnp.dot(x, row_tab[...], preferred_element_type=jnp.float32)
            for b in range(bands):
                half[j, b] = stacked(h[b * GB : (b + 1) * GB])
        return carry

    deep = largest(planes, 3)
    lax.fori_loop(0, planes // deep, rows_of, 0)

    tails = tail.shape[0]
    for t in range(tails):
        js = range(t * SHARE, min(planes, (t + 1) * SHARE))
        x = jnp.concatenate([both[j] for j in js], axis=1)
        h = jnp.dot(x, end_tab[: len(js) * 2 * LANES, :], preferred_element_type=jnp.float32)
        for b in range(bands):
            tail[t, b] = stacked(h[b * GB : (b + 1) * GB])

    wide = largest(bands, 6)

    def columns_of(step, carry):
        pieces = []
        for u in range(wide):
            b = wide * step + u
            pieces += [(acc, j, half, b) for j in range(planes)]
        for t in range(tails):
            pieces += [(acc_tail, t, tail, wide * step + u) for u in range(wide)]
        for i in range(0, len(pieces), 2):
            two = pieces[i : i + 2]
            x = jnp.concatenate([src[j, b] for _, j, src, b in two], axis=1)
            wave = jnp.dot(col_tab[...], x, preferred_element_type=jnp.float32)
            re, im = wave[:N], wave[N:]
            sq = re * re + im * im
            for side, (to, j, _, b) in enumerate(two):
                to[j] = to[j] + sq[:, side * LANES : (side + 1) * LANES] * weight[b]
        return carry

    lax.fori_loop(0, bands // wide, columns_of, 0)

    def deal(mine_bit):
        for o in range(owners):
            to = keep if o % 2 == mine_bit else send
            mine = slice(o * own_rows, (o + 1) * own_rows)
            for j in range(planes):
                to[o // 2, j, :own_rows, :] = acc[j, mine, :].astype(jnp.bfloat16)
            for t in range(tails):
                to[o // 2, planes + t, :own_rows, :] = acc_tail[t, mine, :].astype(jnp.bfloat16)

    @pl.when(core[0] == 0)
    def _():
        deal(0)

    @pl.when(core[0] != 0)
    def _():
        deal(1)


def sum_kernel(planes, own_rows, *refs):
    *parts, out = refs
    base = 0
    for c, count in enumerate(planes):
        total = parts[2 * c][...].astype(jnp.float32) + parts[2 * c + 1][...].astype(jnp.float32)
        for j in range(count):
            at = j % SHARE * TAIL
            out[base + j, :, :LANES] = total[j, :own_rows]
            out[base + j, :, LANES:] = total[count + j // SHARE, :own_rows, at : at + TAIL]
        base += count


def up(n, m):
    return -(-n // m) * m


def largest(n, most):
    return max(d for d in range(1, most + 1) if n % d == 0)


def vmem_call(kernel, out_shape, n_in, scratch=(), flops=1, smem=(), far=()):
    vmem_scratch = [m for m in scratch if m.memory_space == pltpu.VMEM]
    used = sum(math.prod(m.shape) * jnp.dtype(m.dtype).itemsize for m in vmem_scratch)
    vmem = pl.BlockSpec(memory_space=pltpu.VMEM)
    scalar = pl.BlockSpec(memory_space=pltpu.SMEM)
    hbm = pl.BlockSpec(memory_space=pltpu.HBM)
    many = isinstance(out_shape, list)
    return pl.pallas_call(
        kernel,
        out_shape=out_shape,
        in_specs=[scalar if i in smem else hbm if i in far else vmem for i in range(n_in)],
        out_specs=[vmem] * len(out_shape) if many else vmem,
        scratch_shapes=list(scratch),
        compiler_params=pltpu.CompilerParams(vmem_limit_bytes=62 * 2**20 if far else min(62 * 2**20, used + 12 * 2**20)),
        cost_estimate=pl.CostEstimate(flops=flops, bytes_accessed=1 << 20, transcendentals=0),
    )


def partners(axis, bit):
    return [(i, i ^ (1 << bit)) for i in range(lax.axis_size(axis))]


def halve(keep, send, axis):
    bit = 0
    while True:
        got = lax.ppermute(send, axis, partners(axis, bit))
        if keep.shape[0] == 1:
            return keep[0], got[0]
        whole = (keep.astype(jnp.float32) + got.astype(jnp.float32)).astype(keep.dtype)
        bit += 1
        here = lax.axis_index(axis) >> bit & 1
        pairs = whole.reshape((whole.shape[0] // 2, 2) + whole.shape[1:])
        keep = lax.dynamic_index_in_dim(pairs, here, 1, keepdims=False)
        send = lax.dynamic_index_in_dim(pairs, 1 - here, 1, keepdims=False)


def shards(coefficients, occupations, columns, counts, plane_slot):
    bands = coefficients.shape[0]
    ranks = lax.axis_size("fft")
    owners = lax.axis_size("band")
    slots = columns.shape[0]
    held = plane_slot.shape[0] // ranks
    planes = (held // 3, held - held // 3)
    cap = up(ranks * slots * 2 // 5, LANES)
    own_rows = N // owners
    bf16, f32 = jnp.bfloat16, jnp.float32

    weight = occupations / (bands * owners)
    core = (lax.axis_index("band") & 1)[None]
    tables = wave_tables()

    spans = [up(-(-2 * count * bands // GROUPS), 8) for count in planes]
    rows = [2 * count * bands for count in planes]
    fixed = stick_constants(planes, ranks)
    stride = up(slots, 8) + 8
    outgoing = vmem_call(
        functools.partial(stick_kernel, planes, ranks),
        [jax.ShapeDtypeStruct((ranks, rows[0] + spans[0] + INFO, LANES), bf16)]
        + [jax.ShapeDtypeStruct((rows[1] + spans[1], LANES), bf16)] * ranks,
        5,
        [
            pltpu.SMEM(counts.shape, jnp.int32),
            pltpu.VMEM(plane_slot.shape, jnp.int32),
            pltpu.VMEM(fixed.shape, bf16),
            pltpu.VMEM(coefficients.shape, bf16),
            pltpu.VMEM(columns.shape, jnp.int32),
            pltpu.SemaphoreType.DMA((5,)),
        ]
        + [pltpu.VMEM((bands * stride, LANES), f32)] * 2
        + [pltpu.VMEM((INFO, LANES), f32)]
        + [pltpu.VMEM((ranks, GROUPS * span, LANES), f32) for span in spans * 2],
        flops=4 * 10**9,
        far=range(5),
    )(counts, plane_slot, fixed, coefficients, columns)
    kept_shapes = [
        jax.ShapeDtypeStruct((ranks, cap), f32),
        jax.ShapeDtypeStruct((cap, LANES), bf16),
        jax.ShapeDtypeStruct((cap, LANES), bf16),
    ]
    kept, halves = [], []
    for c, (count, span) in enumerate(zip(planes, spans)):
        first = c == 0
        if first:
            received = [lax.all_to_all(outgoing[0], "fft", split_axis=0, concat_axis=0, tiled=True)]
        else:
            received = [outgoing[1]]
            for k in range(1, ranks):
                pairs = [(i, i ^ k) for i in range(ranks)]
                received.append(lax.ppermute(outgoing[1 + k], "fft", pairs))
        tails = -(-count // SHARE)
        dens_shape = jax.ShapeDtypeStruct(
            (owners // 2, count + tails, up(own_rows, 8), LANES), bf16
        )
        run = vmem_call(
            functools.partial(plane_kernel, first, bands, ranks, count, span, owners, own_rows),
            [dens_shape] * 2 + (kept_shapes if first else []),
            len(received) + (5 if first else 8),
            [
                pltpu.VMEM((rows[c] + (INFO if first else 0), ranks * 2 * LANES), bf16),
                pltpu.VMEM((ranks * 2 * LANES, cap), bf16),
                pltpu.VMEM((rows[c], cap), bf16),
                pltpu.VMEM((count * bands * GB, LANES), f32),
                pltpu.VMEM((count * bands * GB, LANES), f32),
                pltpu.VMEM((count, bands * GB, 2 * LANES), bf16),
                pltpu.VMEM((count, bands, 2 * GB, LANES), bf16),
                pltpu.VMEM((tails, bands, 2 * GB, LANES), bf16),
                pltpu.VMEM((count, N, LANES), f32),
                pltpu.VMEM((tails, N, LANES), f32),
            ],
            flops=16 * 10**9,
            smem=(len(received) + 3, len(received) + 4),
        )
        results = run(*received, *tables, weight, core, *kept)
        if first:
            kept = list(results[2:])
        halves += halve(results[0], results[1], "band")
    return vmem_call(
        functools.partial(sum_kernel, planes, own_rows),
        jax.ShapeDtypeStruct((held, own_rows, N), f32),
        len(halves),
    )(*halves)


def solution(mesh):
    placed = (P("band", "fft"), P("band"), P("fft"), P("fft"), P())

    return jax.shard_map(
        shards, mesh=mesh, in_specs=placed, out_specs=P("fft", "band", None), check_vma=False
    )
```

```python
import functools
import math

import jax
import jax.numpy as jnp
import numpy as np
from jax import lax
from jax.experimental import pallas as pl
from jax.experimental.pallas import tpu as pltpu
from jax.sharding import PartitionSpec as P


N = 144
GB = 72
LANES = 128
TAIL = N - LANES
SHARE = LANES // TAIL
PAIRS = 12
INFO = 8
GROUPS = 4


def wave_tables():
    freqs = np.arange(GB) - GB // 2
    angles = (freqs[:, None] * np.arange(N)[None, :] % N) * (2.0 * math.pi / N)
    cosine, sine = np.cos(angles), np.sin(angles)
    rows = np.zeros((2 * LANES, 2 * LANES), np.float32)
    ends = np.zeros((SHARE, 2 * LANES, 2 * LANES), np.float32)
    for col, real_from, imag_from in ((0, cosine, -sine), (1, sine, cosine)):
        rows[:GB, col * LANES : (col + 1) * LANES] = real_from[:, :LANES]
        rows[LANES : LANES + GB, col * LANES : (col + 1) * LANES] = imag_from[:, :LANES]
        for j in range(SHARE):
            at = col * LANES + j * TAIL
            ends[j, :GB, at : at + TAIL] = real_from[:, LANES:]
            ends[j, LANES : LANES + GB, at : at + TAIL] = imag_from[:, LANES:]
    cols = np.block([[cosine.T, -sine.T], [sine.T, cosine.T]])
    ends = ends.reshape(SHARE * 2 * LANES, 2 * LANES)
    return [jnp.asarray(x, jnp.bfloat16) for x in (rows, ends, cols)]


def stick_constants(planes, ranks):
    freqs = np.arange(GB) - GB // 2
    angles = (np.arange(N)[:, None] * freqs[None, :] % N) * (2.0 * math.pi / N)
    cosine, sine = np.cos(angles), np.sin(angles)
    held = sum(planes)
    ordered = sum(ranks * up(2 * count, 8) for count in planes)
    fixed = np.zeros((2, N + ordered, up(max(2 * LANES, ranks * held), LANES)), np.float32)
    fixed[0, :N, : 2 * GB] = np.concatenate([cosine, -sine], axis=1)
    fixed[1, :N, : 2 * GB] = np.concatenate([sine, cosine], axis=1)
    row, base = N, 0
    for count in planes:
        for d in range(ranks):
            for part in range(2):
                for j in range(count):
                    fixed[part, row + part * count + j, d * held + base + j] = 1
            row += up(2 * count, 8)
        base += count
    return jnp.asarray(fixed.reshape(-1, fixed.shape[2]), jnp.bfloat16)


def lane_group(rows, dtype):
    group = lax.broadcasted_iota(jnp.int32, (rows, LANES), 1) // 32
    return [(group == g).astype(jnp.float32).astype(dtype) for g in range(GROUPS)]


def stick_kernel(planes, ranks, *refs):
    chunks = len(planes)
    outs, scratch = refs[5 : 6 + (chunks - 1) * ranks], refs[6 + (chunks - 1) * ranks :]
    me = lax.axis_index("fft")
    count_here, slot_of, fixed, coef, column, done, low, high, ends = scratch[:9]
    mains, rests = scratch[9 : 9 + chunks], scratch[9 + chunks :]
    bands, slots = coef.shape[0], column.shape[0]
    inside = (count_here, slot_of, fixed, coef, column)
    copies = [
        pltpu.make_async_copy(src, to, done.at[i]) for i, (src, to) in enumerate(zip(refs, inside))
    ]
    for copy in copies:
        copy.start()
    for main, rest, count in zip(mains, rests, planes):
        if 2 * count * bands < main.shape[1]:
            main[...] = jnp.zeros_like(main)
            rest[...] = jnp.zeros_like(rest)

    def product(x, y, dims):
        return lax.dot_general(x, y, (dims, ((), ())), preferred_element_type=jnp.float32)

    copies[1].wait()
    copies[2].wait()
    held = slot_of[...].reshape(1, -1)
    at_pos = lax.broadcasted_iota(jnp.int32, (N, held.shape[1]), 0) == held
    at_pos = jnp.where(at_pos, 1.0, 0.0).astype(jnp.bfloat16)
    table = 0.0
    ordered = fixed.shape[0] // 2 - N
    for part in range(2):
        at = part * (N + ordered)
        pos = fixed[at : at + N]
        order = fixed[at + N : at + N + ordered, : held.shape[1]]
        rows_of_slot = product(at_pos, pos, ((0,), (0,))).astype(jnp.bfloat16)
        table = table + product(order, rows_of_slot, ((1,), (0,)))
    table = table.astype(jnp.bfloat16)

    stride = low.shape[0] // bands
    copies[3].wait()
    for s in range(slots):
        tile, shift = divmod(s * 2 * GB, LANES)
        x = coef[:, tile * LANES : (tile + 2) * LANES].astype(jnp.float32)
        if shift:
            x = pltpu.roll(x, 2 * LANES - shift, 1)
        low[pl.ds(s, bands, stride=stride), :] = x[:, :LANES]
        high[pl.ds(s, bands, stride=stride), :] = x[:, LANES:]

    for b in range(bands):
        here = slice(b * stride, b * stride + slots)
        x = jnp.concatenate([low[here], high[here]], axis=1).astype(jnp.bfloat16)
        x = jnp.concatenate([x[:LANES]] + [x[LANES:]] * 4, axis=0)
        val = product(table, x, ((1,), (1,)))
        at = 0
        for main, rest, count in zip(mains, rests, planes):
            for d in range(ranks):
                part = val[at : at + 2 * count]
                main[d, pl.ds(b, 2 * count, stride=bands), :] = part[:, :LANES]
                rest[d, pl.ds(b, 2 * count, stride=bands), :] = part[:, LANES:]
                at += up(2 * count, 8)

    copies[0].wait()
    copies[4].wait()
    c = column[...].reshape(1, -1).astype(jnp.float32)
    gx = jnp.floor((c + 0.5) * (1.0 / GB))
    row = lax.broadcasted_iota(jnp.int32, (INFO, slots), 0)
    live = count_here[0].astype(jnp.float32)
    info = jnp.where(row % 3 == 0, gx, jnp.where(row % 3 == 1, c - GB * gx, live))
    ends[...] = jnp.zeros_like(ends)
    ends[:, : slots - LANES] = info[:, LANES:]
    row = lax.broadcasted_iota(jnp.int32, (INFO, LANES), 0)
    info = jnp.where(row < 3, info[:, :LANES], jnp.where(row < 5, ends[...], 0.0))

    for c, (main, rest, count) in enumerate(zip(mains, rests, planes)):
        rows = 2 * count * bands
        span = main.shape[1] // GROUPS
        masks = lane_group(span, jnp.float32)
        at = rows + (INFO if c == 0 else 0)
        for k in range(ranks):
            out, d = (outs[0].at[k], k) if c == 0 else (outs[1 + (c - 1) * ranks + k], me ^ k)
            out[:rows, :] = main[d, :rows, :].astype(jnp.bfloat16)
            packed = rest[d, :span, :] * masks[0]
            for g in range(1, GROUPS):
                packed = packed + rest[d, g * span : (g + 1) * span, :] * masks[g]
            if c == 0:
                out[rows:at, :] = info.astype(jnp.bfloat16)
            out[at:, :] = packed.astype(jnp.bfloat16)


def plane_kernel(first, bands, ranks, planes, span, owners, own_rows, *refs):
    if first:
        recv, row_tab, end_tab, col_tab, weight, core, keep, send, turn, gx_of, gy_hot = refs[:11]
        blocks, source = [recv.at[src] for src in range(ranks)], lambda k: slice(k, k + 1)
    else:
        blocks, refs = refs[:ranks], refs[ranks - 1 :]
        _, row_tab, end_tab, col_tab, weight, core, turn, gx_of, gy_hot, keep, send = refs[:11]
        me = lax.axis_index("fft")
        source = lambda k: pl.ds(me ^ k, 1)
    lhs, pick, sticks, real, imag, both, half, tail, acc, acc_tail = refs[11:]
    live = planes * bands
    rows = 2 * live
    total = rows + INFO if first else rows
    cap = turn.shape[1]

    if first:
        place = lax.broadcasted_iota(jnp.int32, (1, cap), 1).astype(jnp.float32)
        start = jnp.zeros((1, 1), jnp.float32)
        for src in range(ranks):
            count = blocks[src][rows : rows + INFO, :].astype(jnp.float32)[2:3, 0:1]
            t = place - start
            turn[src : src + 1, :] = jnp.where(jnp.logical_and(t >= 0, t < count), t, -1.0)
            start = start + count

    masks = lane_group(span, jnp.bfloat16)
    k = lax.broadcasted_iota(jnp.int32, (2 * LANES, cap), 0)
    slot = jnp.where(k < LANES, k, LANES + k % 32).astype(jnp.float32).astype(jnp.bfloat16)
    one, zero = jnp.ones((), jnp.bfloat16), jnp.zeros((), jnp.bfloat16)
    if first:
        info_row = lax.broadcasted_iota(jnp.int32, (INFO, LANES), 0)
        info_main = (info_row < 3).astype(jnp.float32).astype(jnp.bfloat16)
    for src in range(ranks):
        at = src * 2 * LANES
        wanted = jnp.broadcast_to(turn[source(src), :].astype(jnp.bfloat16), slot.shape)
        pick[at : at + 2 * LANES, :] = jnp.where(slot == wanted, one, zero)
        block, low, high = blocks[src], slice(at, at + LANES), slice(at + LANES, at + 2 * LANES)
        lhs[:rows, low] = block[:rows, :]
        packed = block[total : total + span, :]
        for g in range(GROUPS):
            here = slice(g * span, min(rows, (g + 1) * span))
            if here.start < here.stop:
                lhs[here, high] = (packed * masks[g])[: here.stop - here.start]
        if first:
            info = block[rows:total, :]
            lhs[rows:, low] = info * info_main
            lhs[rows:, high] = info * (one - info_main)
    compact = jnp.dot(lhs[...], pick[...], preferred_element_type=jnp.float32)
    sticks[...] = compact[:rows].astype(jnp.bfloat16)

    if first:
        info = jnp.concatenate(
            [compact[rows:], jnp.zeros((LANES - INFO, cap), jnp.float32)], axis=0
        ).T
        lane = lax.broadcasted_iota(jnp.int32, (cap, LANES), 1).astype(jnp.float32)
        gx, gy = (info[:, i : i + 1] + info[:, i + 3 : i + 4] for i in range(2))
        gx_of[...] = jnp.broadcast_to(gx, (cap, LANES)).astype(jnp.bfloat16)
        gy_hot[...] = jnp.where(gy == lane, 1.0, 0.0).astype(jnp.bfloat16)

    def put(step, carry):
        for u in range(PAIRS):
            pair = PAIRS * step + u
            hot = []
            for side in range(2):
                gx = (2 * pair + side).astype(jnp.float32).astype(jnp.bfloat16)
                hot.append(jnp.where(gx_of[...] == gx, gy_hot[...], jnp.zeros((), jnp.bfloat16)))
            placed = jnp.dot(
                sticks[...], jnp.concatenate(hot, axis=1), preferred_element_type=jnp.float32
            )
            for side in range(2):
                lanes = slice(side * LANES, (side + 1) * LANES)
                at = 2 * pair + side
                real[pl.ds(at, live, stride=GB), :] = placed[:live, lanes]
                imag[pl.ds(at, live, stride=GB), :] = placed[live : 2 * live, lanes]
        return carry

    lax.fori_loop(0, GB // 2 // PAIRS, put, 0)

    acc[...] = jnp.zeros_like(acc)
    acc_tail[...] = jnp.zeros_like(acc_tail)

    def stacked(piece):
        return jnp.concatenate([piece[:, :LANES], piece[:, LANES:]], axis=0).astype(jnp.bfloat16)

    def rows_of(first_plane, count):
        for u in range(count):
            j = first_plane + u
            at = j * (bands * GB)
            at = at if isinstance(at, int) else pl.multiple_of(at, 8)
            at = pl.ds(at, bands * GB)
            x = jnp.concatenate(
                [real[at, :].astype(jnp.bfloat16), imag[at, :].astype(jnp.bfloat16)], axis=1
            )
            both[j] = x
            h = jnp.dot(x, row_tab[...], preferred_element_type=jnp.float32)
            for b in range(bands):
                half[j, b] = stacked(h[b * GB : (b + 1) * GB])

    deep = min(planes, 3)
    lax.fori_loop(0, planes // deep, lambda step, _: rows_of(step * deep, deep), None)
    rows_of(planes - planes % deep, planes % deep)

    tails = tail.shape[0]
    for t in range(tails):
        js = range(t * SHARE, min(planes, (t + 1) * SHARE))
        x = jnp.concatenate([both[j] for j in js], axis=1)
        h = jnp.dot(x, end_tab[: len(js) * 2 * LANES, :], preferred_element_type=jnp.float32)
        for b in range(bands):
            tail[t, b] = stacked(h[b * GB : (b + 1) * GB])

    wide = largest(bands, 6)

    def columns_of(step, carry):
        pieces = []
        for u in range(wide):
            b = wide * step + u
            pieces += [(acc, j, half, b) for j in range(planes)]
        for t in range(tails):
            pieces += [(acc_tail, t, tail, wide * step + u) for u in range(wide)]
        for i in range(0, len(pieces), 2):
            two = pieces[i : i + 2]
            x = jnp.concatenate([src[j, b] for _, j, src, b in two], axis=1)
            wave = jnp.dot(col_tab[...], x, preferred_element_type=jnp.float32)
            re, im = wave[:N], wave[N:]
            sq = re * re + im * im
            for side, (to, j, _, b) in enumerate(two):
                to[j] = to[j] + sq[:, side * LANES : (side + 1) * LANES] * weight[b]
        return carry

    lax.fori_loop(0, bands // wide, columns_of, 0)

    def deal(mine_bit):
        for o in range(owners):
            to = keep if o % 2 == mine_bit else send
            mine = slice(o * own_rows, (o + 1) * own_rows)
            for j in range(planes):
                to[o // 2, j, :own_rows, :] = acc[j, mine, :].astype(jnp.bfloat16)
            for t in range(tails):
                to[o // 2, planes + t, :own_rows, :] = acc_tail[t, mine, :].astype(jnp.bfloat16)

    @pl.when(core[0] == 0)
    def _():
        deal(0)

    @pl.when(core[0] != 0)
    def _():
        deal(1)


def sum_kernel(planes, own_rows, *refs):
    *parts, out = refs
    base = 0
    for c, count in enumerate(planes):
        total = parts[2 * c][...].astype(jnp.float32) + parts[2 * c + 1][...].astype(jnp.float32)
        for j in range(count):
            at = j % SHARE * TAIL
            out[base + j, :, :LANES] = total[j, :own_rows]
            out[base + j, :, LANES:] = total[count + j // SHARE, :own_rows, at : at + TAIL]
        base += count


def up(n, m):
    return -(-n // m) * m


def largest(n, most):
    return max(d for d in range(1, most + 1) if n % d == 0)


def vmem_call(kernel, out_shape, n_in, scratch=(), flops=1, smem=(), far=()):
    vmem_scratch = [m for m in scratch if m.memory_space == pltpu.VMEM]
    used = sum(math.prod(m.shape) * jnp.dtype(m.dtype).itemsize for m in vmem_scratch)
    vmem = pl.BlockSpec(memory_space=pltpu.VMEM)
    scalar = pl.BlockSpec(memory_space=pltpu.SMEM)
    hbm = pl.BlockSpec(memory_space=pltpu.HBM)
    many = isinstance(out_shape, list)
    return pl.pallas_call(
        kernel,
        out_shape=out_shape,
        in_specs=[scalar if i in smem else hbm if i in far else vmem for i in range(n_in)],
        out_specs=[vmem] * len(out_shape) if many else vmem,
        scratch_shapes=list(scratch),
        compiler_params=pltpu.CompilerParams(vmem_limit_bytes=62 * 2**20 if far else min(62 * 2**20, used + 12 * 2**20)),
        cost_estimate=pl.CostEstimate(flops=flops, bytes_accessed=1 << 20, transcendentals=0),
    )


def partners(axis, bit):
    return [(i, i ^ (1 << bit)) for i in range(lax.axis_size(axis))]


def halve(keep, send, axis):
    bit = 0
    while True:
        got = lax.ppermute(send, axis, partners(axis, bit))
        if keep.shape[0] == 1:
            return keep[0], got[0]
        whole = (keep.astype(jnp.float32) + got.astype(jnp.float32)).astype(keep.dtype)
        bit += 1
        here = lax.axis_index(axis) >> bit & 1
        pairs = whole.reshape((whole.shape[0] // 2, 2) + whole.shape[1:])
        keep = lax.dynamic_index_in_dim(pairs, here, 1, keepdims=False)
        send = lax.dynamic_index_in_dim(pairs, 1 - here, 1, keepdims=False)


def shards(coefficients, occupations, columns, counts, plane_slot):
    bands = coefficients.shape[0]
    ranks = lax.axis_size("fft")
    owners = lax.axis_size("band")
    slots = columns.shape[0]
    held = plane_slot.shape[0] // ranks
    planes = (held // 3, held - held // 3)
    cap = up(ranks * slots * 2 // 5, LANES)
    own_rows = N // owners
    bf16, f32 = jnp.bfloat16, jnp.float32

    weight = occupations / (bands * owners)
    core = (lax.axis_index("band") & 1)[None]
    tables = wave_tables()

    spans = [up(-(-2 * count * bands // GROUPS), 8) for count in planes]
    rows = [2 * count * bands for count in planes]
    fixed = stick_constants(planes, ranks)
    stride = up(slots, 8) + 8
    outgoing = vmem_call(
        functools.partial(stick_kernel, planes, ranks),
        [jax.ShapeDtypeStruct((ranks, rows[0] + spans[0] + INFO, LANES), bf16)]
        + [jax.ShapeDtypeStruct((rows[1] + spans[1], LANES), bf16)] * ranks,
        5,
        [
            pltpu.SMEM(counts.shape, jnp.int32),
            pltpu.VMEM(plane_slot.shape, jnp.int32),
            pltpu.VMEM(fixed.shape, bf16),
            pltpu.VMEM(coefficients.shape, bf16),
            pltpu.VMEM(columns.shape, jnp.int32),
            pltpu.SemaphoreType.DMA((5,)),
        ]
        + [pltpu.VMEM((bands * stride, LANES), f32)] * 2
        + [pltpu.VMEM((INFO, LANES), f32)]
        + [pltpu.VMEM((ranks, GROUPS * span, LANES), f32) for span in spans * 2],
        flops=4 * 10**9,
        far=range(5),
    )(counts, plane_slot, fixed, coefficients, columns)
    kept_shapes = [
        jax.ShapeDtypeStruct((ranks, cap), f32),
        jax.ShapeDtypeStruct((cap, LANES), bf16),
        jax.ShapeDtypeStruct((cap, LANES), bf16),
    ]
    kept, halves = [], []
    for c, (count, span) in enumerate(zip(planes, spans)):
        first = c == 0
        if first:
            received = [lax.all_to_all(outgoing[0], "fft", split_axis=0, concat_axis=0, tiled=True)]
        else:
            received = [outgoing[1]]
            for k in range(1, ranks):
                pairs = [(i, i ^ k) for i in range(ranks)]
                received.append(lax.ppermute(outgoing[1 + k], "fft", pairs))
        tails = -(-count // SHARE)
        dens_shape = jax.ShapeDtypeStruct(
            (owners // 2, count + tails, up(own_rows, 8), LANES), bf16
        )
        run = vmem_call(
            functools.partial(plane_kernel, first, bands, ranks, count, span, owners, own_rows),
            [dens_shape] * 2 + (kept_shapes if first else []),
            len(received) + (5 if first else 8),
            [
                pltpu.VMEM((rows[c] + (INFO if first else 0), ranks * 2 * LANES), bf16),
                pltpu.VMEM((ranks * 2 * LANES, cap), bf16),
                pltpu.VMEM((rows[c], cap), bf16),
                pltpu.VMEM((count * bands * GB, LANES), f32),
                pltpu.VMEM((count * bands * GB, LANES), f32),
                pltpu.VMEM((count, bands * GB, 2 * LANES), bf16),
                pltpu.VMEM((count, bands, 2 * GB, LANES), bf16),
                pltpu.VMEM((tails, bands, 2 * GB, LANES), bf16),
                pltpu.VMEM((count, N, LANES), f32),
                pltpu.VMEM((tails, N, LANES), f32),
            ],
            flops=16 * 10**9,
            smem=(len(received) + 3, len(received) + 4),
        )
        results = run(*received, *tables, weight, core, *kept)
        if first:
            kept = list(results[2:])
        halves += halve(results[0], results[1], "band")
    return vmem_call(
        functools.partial(sum_kernel, planes, own_rows),
        jax.ShapeDtypeStruct((held, own_rows, N), f32),
        len(halves),
    )(*halves)


def solution(mesh):
    placed = (P("band", "fft"), P("band"), P("fft"), P("fft"), P())

    return jax.shard_map(
        shards, mesh=mesh, in_specs=placed, out_specs=P("fft", "band", None), check_vma=False
    )
```

```python
import functools
import math

import jax
import jax.numpy as jnp
import numpy as np
from jax import lax
from jax.experimental import pallas as pl
from jax.experimental.pallas import tpu as pltpu
from jax.sharding import PartitionSpec as P


N = 144
GB = 72
LANES = 128
TAIL = N - LANES
SHARE = LANES // TAIL
PAIRS = 18
INFO = 8
GROUPS = 4


def wave_tables():
    freqs = np.arange(GB) - GB // 2
    angles = (freqs[:, None] * np.arange(N)[None, :] % N) * (2.0 * math.pi / N)
    cosine, sine = np.cos(angles), np.sin(angles)
    rows = np.zeros((2 * LANES, 2 * LANES), np.float32)
    ends = np.zeros((SHARE, 2 * LANES, 2 * LANES), np.float32)
    for col, real_from, imag_from in ((0, cosine, -sine), (1, sine, cosine)):
        rows[:GB, col * LANES : (col + 1) * LANES] = real_from[:, :LANES]
        rows[LANES : LANES + GB, col * LANES : (col + 1) * LANES] = imag_from[:, :LANES]
        for j in range(SHARE):
            at = col * LANES + j * TAIL
            ends[j, :GB, at : at + TAIL] = real_from[:, LANES:]
            ends[j, LANES : LANES + GB, at : at + TAIL] = imag_from[:, LANES:]
    cols = np.block([[cosine.T, -sine.T], [sine.T, cosine.T]])
    ends = ends.reshape(SHARE * 2 * LANES, 2 * LANES)
    return [jnp.asarray(x, jnp.bfloat16) for x in (rows, ends, cols)]


def stick_constants(planes, ranks):
    freqs = np.arange(GB) - GB // 2
    angles = (np.arange(N)[:, None] * freqs[None, :] % N) * (2.0 * math.pi / N)
    cosine, sine = np.cos(angles), np.sin(angles)
    held = sum(planes)
    ordered = sum(ranks * up(2 * count, 8) for count in planes)
    fixed = np.zeros((2, N + ordered, up(max(2 * LANES, ranks * held), LANES)), np.float32)
    fixed[0, :N, : 2 * GB] = np.concatenate([cosine, -sine], axis=1)
    fixed[1, :N, : 2 * GB] = np.concatenate([sine, cosine], axis=1)
    row, base = N, 0
    for count in planes:
        for d in range(ranks):
            for part in range(2):
                for j in range(count):
                    fixed[part, row + part * count + j, d * held + base + j] = 1
            row += up(2 * count, 8)
        base += count
    return jnp.asarray(fixed.reshape(-1, fixed.shape[2]), jnp.bfloat16)


def lane_group(rows, dtype):
    group = lax.broadcasted_iota(jnp.int32, (rows, LANES), 1) // 32
    return [(group == g).astype(jnp.float32).astype(dtype) for g in range(GROUPS)]


def stick_kernel(planes, ranks, *refs):
    chunks = len(planes)
    outs, scratch = refs[5 : 6 + (chunks - 1) * ranks], refs[6 + (chunks - 1) * ranks :]
    me = lax.axis_index("fft")
    count_here, slot_of, fixed, coef, column, done, low, high, ends = scratch[:9]
    mains, rests = scratch[9 : 9 + chunks], scratch[9 + chunks :]
    bands, slots = coef.shape[0], column.shape[0]
    inside = (count_here, slot_of, fixed, coef, column)
    copies = [
        pltpu.make_async_copy(src, to, done.at[i]) for i, (src, to) in enumerate(zip(refs, inside))
    ]
    for copy in copies:
        copy.start()
    for main, rest, count in zip(mains, rests, planes):
        if 2 * count * bands < main.shape[1]:
            main[...] = jnp.zeros_like(main)
            rest[...] = jnp.zeros_like(rest)

    def product(x, y, dims):
        return lax.dot_general(x, y, (dims, ((), ())), preferred_element_type=jnp.float32)

    copies[1].wait()
    copies[2].wait()
    held = slot_of[...].reshape(1, -1)
    at_pos = lax.broadcasted_iota(jnp.int32, (N, held.shape[1]), 0) == held
    at_pos = jnp.where(at_pos, 1.0, 0.0).astype(jnp.bfloat16)
    table = 0.0
    ordered = fixed.shape[0] // 2 - N
    for part in range(2):
        at = part * (N + ordered)
        pos = fixed[at : at + N]
        order = fixed[at + N : at + N + ordered, : held.shape[1]]
        rows_of_slot = product(at_pos, pos, ((0,), (0,))).astype(jnp.bfloat16)
        table = table + product(order, rows_of_slot, ((1,), (0,)))
    table = table.astype(jnp.bfloat16)

    stride = low.shape[0] // bands
    copies[3].wait()
    for s in range(slots):
        tile, shift = divmod(s * 2 * GB, LANES)
        x = coef[:, tile * LANES : (tile + 2) * LANES].astype(jnp.float32)
        if shift:
            x = pltpu.roll(x, 2 * LANES - shift, 1)
        low[pl.ds(s, bands, stride=stride), :] = x[:, :LANES]
        high[pl.ds(s, bands, stride=stride), :] = x[:, LANES:]

    for b in range(bands):
        here = slice(b * stride, b * stride + slots)
        x = jnp.concatenate([low[here], high[here]], axis=1).astype(jnp.bfloat16)
        x = jnp.concatenate([x[:LANES]] + [x[LANES:]] * 4, axis=0)
        val = product(table, x, ((1,), (1,)))
        at = 0
        for main, rest, count in zip(mains, rests, planes):
            for d in range(ranks):
                part = val[at : at + 2 * count]
                main[d, pl.ds(b, 2 * count, stride=bands), :] = part[:, :LANES]
                rest[d, pl.ds(b, 2 * count, stride=bands), :] = part[:, LANES:]
                at += up(2 * count, 8)

    copies[0].wait()
    copies[4].wait()
    c = column[...].reshape(1, -1).astype(jnp.float32)
    gx = jnp.floor((c + 0.5) * (1.0 / GB))
    row = lax.broadcasted_iota(jnp.int32, (INFO, slots), 0)
    live = count_here[0].astype(jnp.float32)
    info = jnp.where(row % 3 == 0, gx, jnp.where(row % 3 == 1, c - GB * gx, live))
    ends[...] = jnp.zeros_like(ends)
    ends[:, : slots - LANES] = info[:, LANES:]
    row = lax.broadcasted_iota(jnp.int32, (INFO, LANES), 0)
    info = jnp.where(row < 3, info[:, :LANES], jnp.where(row < 5, ends[...], 0.0))

    for c, (main, rest, count) in enumerate(zip(mains, rests, planes)):
        rows = 2 * count * bands
        span = main.shape[1] // GROUPS
        masks = lane_group(span, jnp.float32)
        at = rows + (INFO if c == 0 else 0)
        for k in range(ranks):
            out, d = (outs[0].at[k], k) if c == 0 else (outs[1 + (c - 1) * ranks + k], me ^ k)
            out[:rows, :] = main[d, :rows, :].astype(jnp.bfloat16)
            packed = rest[d, :span, :] * masks[0]
            for g in range(1, GROUPS):
                packed = packed + rest[d, g * span : (g + 1) * span, :] * masks[g]
            if c == 0:
                out[rows:at, :] = info.astype(jnp.bfloat16)
            out[at:, :] = packed.astype(jnp.bfloat16)


def plane_kernel(first, bands, ranks, planes, span, owners, own_rows, *refs):
    if first:
        recv, row_tab, end_tab, col_tab, weight, core, keep, send, turn, gx_of, gy_hot = refs[:11]
        blocks, source = [recv.at[src] for src in range(ranks)], lambda k: slice(k, k + 1)
    else:
        blocks, refs = refs[:ranks], refs[ranks - 1 :]
        _, row_tab, end_tab, col_tab, weight, core, turn, gx_of, gy_hot, keep, send = refs[:11]
        me = lax.axis_index("fft")
        source = lambda k: pl.ds(me ^ k, 1)
    lhs, pick, sticks, real, imag, both, half, tail, acc, acc_tail = refs[11:]
    live = planes * bands
    rows = 2 * live
    total = rows + INFO if first else rows
    cap = turn.shape[1]

    if first:
        place = lax.broadcasted_iota(jnp.int32, (1, cap), 1).astype(jnp.float32)
        start = jnp.zeros((1, 1), jnp.float32)
        for src in range(ranks):
            count = blocks[src][rows : rows + INFO, :].astype(jnp.float32)[2:3, 0:1]
            t = place - start
            turn[src : src + 1, :] = jnp.where(jnp.logical_and(t >= 0, t < count), t, -1.0)
            start = start + count

    masks = lane_group(span, jnp.bfloat16)
    k = lax.broadcasted_iota(jnp.int32, (2 * LANES, cap), 0)
    slot = jnp.where(k < LANES, k, LANES + k % 32).astype(jnp.float32).astype(jnp.bfloat16)
    one, zero = jnp.ones((), jnp.bfloat16), jnp.zeros((), jnp.bfloat16)
    if first:
        info_row = lax.broadcasted_iota(jnp.int32, (INFO, LANES), 0)
        info_main = (info_row < 3).astype(jnp.float32).astype(jnp.bfloat16)
    for src in range(ranks):
        at = src * 2 * LANES
        wanted = jnp.broadcast_to(turn[source(src), :].astype(jnp.bfloat16), slot.shape)
        pick[at : at + 2 * LANES, :] = jnp.where(slot == wanted, one, zero)
        block, low, high = blocks[src], slice(at, at + LANES), slice(at + LANES, at + 2 * LANES)
        lhs[:rows, low] = block[:rows, :]
        packed = block[total : total + span, :]
        for g in range(GROUPS):
            here = slice(g * span, min(rows, (g + 1) * span))
            if here.start < here.stop:
                lhs[here, high] = (packed * masks[g])[: here.stop - here.start]
        if first:
            info = block[rows:total, :]
            lhs[rows:, low] = info * info_main
            lhs[rows:, high] = info * (one - info_main)
    compact = jnp.dot(lhs[...], pick[...], preferred_element_type=jnp.float32)
    sticks[...] = compact[:rows].astype(jnp.bfloat16)

    if first:
        info = jnp.concatenate(
            [compact[rows:], jnp.zeros((LANES - INFO, cap), jnp.float32)], axis=0
        ).T
        lane = lax.broadcasted_iota(jnp.int32, (cap, LANES), 1).astype(jnp.float32)
        gx, gy = (info[:, i : i + 1] + info[:, i + 3 : i + 4] for i in range(2))
        gx_of[...] = jnp.broadcast_to(gx, (cap, LANES)).astype(jnp.bfloat16)
        gy_hot[...] = jnp.where(gy == lane, 1.0, 0.0).astype(jnp.bfloat16)

    def put(step, carry):
        for u in range(PAIRS):
            pair = PAIRS * step + u
            hot = []
            for side in range(2):
                gx = (2 * pair + side).astype(jnp.float32).astype(jnp.bfloat16)
                hot.append(jnp.where(gx_of[...] == gx, gy_hot[...], jnp.zeros((), jnp.bfloat16)))
            placed = jnp.dot(
                sticks[...], jnp.concatenate(hot, axis=1), preferred_element_type=jnp.float32
            )
            for side in range(2):
                lanes = slice(side * LANES, (side + 1) * LANES)
                at = 2 * pair + side
                real[pl.ds(at, live, stride=GB), :] = placed[:live, lanes]
                imag[pl.ds(at, live, stride=GB), :] = placed[live : 2 * live, lanes]
        return carry

    lax.fori_loop(0, GB // 2 // PAIRS, put, 0)

    acc[...] = jnp.zeros_like(acc)
    acc_tail[...] = jnp.zeros_like(acc_tail)

    def stacked(piece):
        return jnp.concatenate([piece[:, :LANES], piece[:, LANES:]], axis=0).astype(jnp.bfloat16)

    def rows_of(first_plane, count):
        for u in range(count):
            j = first_plane + u
            at = j * (bands * GB)
            at = at if isinstance(at, int) else pl.multiple_of(at, 8)
            at = pl.ds(at, bands * GB)
            x = jnp.concatenate(
                [real[at, :].astype(jnp.bfloat16), imag[at, :].astype(jnp.bfloat16)], axis=1
            )
            both[j] = x
            h = jnp.dot(x, row_tab[...], preferred_element_type=jnp.float32)
            for b in range(bands):
                half[j, b] = stacked(h[b * GB : (b + 1) * GB])

    deep = min(planes, 12)
    lax.fori_loop(0, planes // deep, lambda step, _: rows_of(step * deep, deep), None)
    rows_of(planes - planes % deep, planes % deep)

    tails = tail.shape[0]
    for t in range(tails):
        js = range(t * SHARE, min(planes, (t + 1) * SHARE))
        x = jnp.concatenate([both[j] for j in js], axis=1)
        h = jnp.dot(x, end_tab[: len(js) * 2 * LANES, :], preferred_element_type=jnp.float32)
        for b in range(bands):
            tail[t, b] = stacked(h[b * GB : (b + 1) * GB])

    wide = largest(bands, 12)

    def columns_of(step, carry):
        pieces = []
        for u in range(wide):
            b = wide * step + u
            pieces += [(acc, j, half, b) for j in range(planes)]
        for t in range(tails):
            pieces += [(acc_tail, t, tail, wide * step + u) for u in range(wide)]
        for i in range(0, len(pieces), 2):
            two = pieces[i : i + 2]
            x = jnp.concatenate([src[j, b] for _, j, src, b in two], axis=1)
            wave = jnp.dot(col_tab[...], x, preferred_element_type=jnp.float32)
            re, im = wave[:N], wave[N:]
            sq = re * re + im * im
            for side, (to, j, _, b) in enumerate(two):
                to[j] = to[j] + sq[:, side * LANES : (side + 1) * LANES] * weight[b]
        return carry

    lax.fori_loop(0, bands // wide, columns_of, 0)

    def deal(mine_bit):
        for o in range(owners):
            to = keep if o % 2 == mine_bit else send
            mine = slice(o * own_rows, (o + 1) * own_rows)
            for j in range(planes):
                to[o // 2, j, :own_rows, :] = acc[j, mine, :].astype(jnp.bfloat16)
            for t in range(tails):
                to[o // 2, planes + t, :own_rows, :] = acc_tail[t, mine, :].astype(jnp.bfloat16)

    @pl.when(core[0] == 0)
    def _():
        deal(0)

    @pl.when(core[0] != 0)
    def _():
        deal(1)


def sum_kernel(planes, own_rows, *refs):
    *parts, out = refs
    base = 0
    for c, count in enumerate(planes):
        total = parts[2 * c][...].astype(jnp.float32) + parts[2 * c + 1][...].astype(jnp.float32)
        for j in range(count):
            at = j % SHARE * TAIL
            out[base + j, :, :LANES] = total[j, :own_rows]
            out[base + j, :, LANES:] = total[count + j // SHARE, :own_rows, at : at + TAIL]
        base += count


def up(n, m):
    return -(-n // m) * m


def largest(n, most):
    return max(d for d in range(1, most + 1) if n % d == 0)


def vmem_call(kernel, out_shape, n_in, scratch=(), flops=1, smem=(), far=()):
    vmem_scratch = [m for m in scratch if m.memory_space == pltpu.VMEM]
    used = sum(math.prod(m.shape) * jnp.dtype(m.dtype).itemsize for m in vmem_scratch)
    vmem = pl.BlockSpec(memory_space=pltpu.VMEM)
    scalar = pl.BlockSpec(memory_space=pltpu.SMEM)
    hbm = pl.BlockSpec(memory_space=pltpu.HBM)
    many = isinstance(out_shape, list)
    return pl.pallas_call(
        kernel,
        out_shape=out_shape,
        in_specs=[scalar if i in smem else hbm if i in far else vmem for i in range(n_in)],
        out_specs=[vmem] * len(out_shape) if many else vmem,
        scratch_shapes=list(scratch),
        compiler_params=pltpu.CompilerParams(vmem_limit_bytes=62 * 2**20 if far else min(62 * 2**20, used + 12 * 2**20)),
        cost_estimate=pl.CostEstimate(flops=flops, bytes_accessed=1 << 20, transcendentals=0),
    )


def partners(axis, bit):
    return [(i, i ^ (1 << bit)) for i in range(lax.axis_size(axis))]


def halve(keep, send, axis):
    bit = 0
    while True:
        got = lax.ppermute(send, axis, partners(axis, bit))
        if keep.shape[0] == 1:
            return keep[0], got[0]
        whole = (keep.astype(jnp.float32) + got.astype(jnp.float32)).astype(keep.dtype)
        bit += 1
        here = lax.axis_index(axis) >> bit & 1
        pairs = whole.reshape((whole.shape[0] // 2, 2) + whole.shape[1:])
        keep = lax.dynamic_index_in_dim(pairs, here, 1, keepdims=False)
        send = lax.dynamic_index_in_dim(pairs, 1 - here, 1, keepdims=False)


def shards(coefficients, occupations, columns, counts, plane_slot):
    bands = coefficients.shape[0]
    ranks = lax.axis_size("fft")
    owners = lax.axis_size("band")
    slots = columns.shape[0]
    held = plane_slot.shape[0] // ranks
    planes = (held // 3, held - held // 3)
    cap = up(ranks * slots * 2 // 5, LANES)
    own_rows = N // owners
    bf16, f32 = jnp.bfloat16, jnp.float32

    weight = occupations / (bands * owners)
    core = (lax.axis_index("band") & 1)[None]
    tables = wave_tables()

    spans = [up(-(-2 * count * bands // GROUPS), 8) for count in planes]
    rows = [2 * count * bands for count in planes]
    fixed = stick_constants(planes, ranks)
    stride = up(slots, 8) + 8
    outgoing = vmem_call(
        functools.partial(stick_kernel, planes, ranks),
        [jax.ShapeDtypeStruct((ranks, rows[0] + spans[0] + INFO, LANES), bf16)]
        + [jax.ShapeDtypeStruct((rows[1] + spans[1], LANES), bf16)] * ranks,
        5,
        [
            pltpu.SMEM(counts.shape, jnp.int32),
            pltpu.VMEM(plane_slot.shape, jnp.int32),
            pltpu.VMEM(fixed.shape, bf16),
            pltpu.VMEM(coefficients.shape, bf16),
            pltpu.VMEM(columns.shape, jnp.int32),
            pltpu.SemaphoreType.DMA((5,)),
        ]
        + [pltpu.VMEM((bands * stride, LANES), f32)] * 2
        + [pltpu.VMEM((INFO, LANES), f32)]
        + [pltpu.VMEM((ranks, GROUPS * span, LANES), f32) for span in spans * 2],
        flops=4 * 10**9,
        far=range(5),
    )(counts, plane_slot, fixed, coefficients, columns)
    kept_shapes = [
        jax.ShapeDtypeStruct((ranks, cap), f32),
        jax.ShapeDtypeStruct((cap, LANES), bf16),
        jax.ShapeDtypeStruct((cap, LANES), bf16),
    ]
    kept, halves = [], []
    for c, (count, span) in enumerate(zip(planes, spans)):
        first = c == 0
        if first:
            received = [lax.all_to_all(outgoing[0], "fft", split_axis=0, concat_axis=0, tiled=True)]
        else:
            received = [outgoing[1]]
            for k in range(1, ranks):
                pairs = [(i, i ^ k) for i in range(ranks)]
                received.append(lax.ppermute(outgoing[1 + k], "fft", pairs))
        tails = -(-count // SHARE)
        dens_shape = jax.ShapeDtypeStruct(
            (owners // 2, count + tails, up(own_rows, 8), LANES), bf16
        )
        run = vmem_call(
            functools.partial(plane_kernel, first, bands, ranks, count, span, owners, own_rows),
            [dens_shape] * 2 + (kept_shapes if first else []),
            len(received) + (5 if first else 8),
            [
                pltpu.VMEM((rows[c] + (INFO if first else 0), ranks * 2 * LANES), bf16),
                pltpu.VMEM((ranks * 2 * LANES, cap), bf16),
                pltpu.VMEM((rows[c], cap), bf16),
                pltpu.VMEM((count * bands * GB, LANES), f32),
                pltpu.VMEM((count * bands * GB, LANES), f32),
                pltpu.VMEM((count, bands * GB, 2 * LANES), bf16),
                pltpu.VMEM((count, bands, 2 * GB, LANES), bf16),
                pltpu.VMEM((tails, bands, 2 * GB, LANES), bf16),
                pltpu.VMEM((count, N, LANES), f32),
                pltpu.VMEM((tails, N, LANES), f32),
            ],
            flops=16 * 10**9,
            smem=(len(received) + 3, len(received) + 4),
        )
        results = run(*received, *tables, weight, core, *kept)
        if first:
            kept = list(results[2:])
        halves += halve(results[0], results[1], "band")
    return vmem_call(
        functools.partial(sum_kernel, planes, own_rows),
        jax.ShapeDtypeStruct((held, own_rows, N), f32),
        len(halves),
    )(*halves)


def solution(mesh):
    placed = (P("band", "fft"), P("band"), P("fft"), P("fft"), P())

    return jax.shard_map(
        shards, mesh=mesh, in_specs=placed, out_specs=P("fft", "band", None), check_vma=False
    )
```

```python
import functools
import math

import jax
import jax.numpy as jnp
import numpy as np
from jax import lax
from jax.experimental import pallas as pl
from jax.experimental.pallas import tpu as pltpu
from jax.sharding import PartitionSpec as P


N = 144
GB = 72
LANES = 128
TAIL = N - LANES
SHARE = LANES // TAIL
PAIRS = 18
INFO = 8
GROUPS = 4


def wave_tables():
    freqs = np.arange(GB) - GB // 2
    angles = (freqs[:, None] * np.arange(N)[None, :] % N) * (2.0 * math.pi / N)
    cosine, sine = np.cos(angles), np.sin(angles)
    rows = np.zeros((2 * LANES, 2 * LANES), np.float32)
    ends = np.zeros((SHARE, 2 * LANES, 2 * LANES), np.float32)
    for col, real_from, imag_from in ((0, cosine, -sine), (1, sine, cosine)):
        rows[:GB, col * LANES : (col + 1) * LANES] = real_from[:, :LANES]
        rows[LANES : LANES + GB, col * LANES : (col + 1) * LANES] = imag_from[:, :LANES]
        for j in range(SHARE):
            at = col * LANES + j * TAIL
            ends[j, :GB, at : at + TAIL] = real_from[:, LANES:]
            ends[j, LANES : LANES + GB, at : at + TAIL] = imag_from[:, LANES:]
    cols = np.block([[cosine.T, -sine.T], [sine.T, cosine.T]])
    ends = ends.reshape(SHARE * 2 * LANES, 2 * LANES)
    return [jnp.asarray(x, jnp.bfloat16) for x in (rows, ends, cols)]


def stick_constants(planes, ranks):
    freqs = np.arange(GB) - GB // 2
    angles = (np.arange(N)[:, None] * freqs[None, :] % N) * (2.0 * math.pi / N)
    cosine, sine = np.cos(angles), np.sin(angles)
    held = sum(planes)
    ordered = sum(ranks * up(2 * count, 8) for count in planes)
    fixed = np.zeros((2, N + ordered, up(max(2 * LANES, ranks * held), LANES)), np.float32)
    fixed[0, :N, : 2 * GB] = np.concatenate([cosine, -sine], axis=1)
    fixed[1, :N, : 2 * GB] = np.concatenate([sine, cosine], axis=1)
    row, base = N, 0
    for count in planes:
        for d in range(ranks):
            for part in range(2):
                for j in range(count):
                    fixed[part, row + part * count + j, d * held + base + j] = 1
            row += up(2 * count, 8)
        base += count
    return jnp.asarray(fixed.reshape(-1, fixed.shape[2]), jnp.bfloat16)


def lane_group(rows, dtype):
    group = lax.broadcasted_iota(jnp.int32, (rows, LANES), 1) // 32
    return [(group == g).astype(jnp.float32).astype(dtype) for g in range(GROUPS)]


def stick_kernel(planes, ranks, *refs):
    chunks = len(planes)
    outs, scratch = refs[5 : 6 + (chunks - 1) * ranks], refs[6 + (chunks - 1) * ranks :]
    me = lax.axis_index("fft")
    count_here, slot_of, fixed, coef, column, done, low, high, ends = scratch[:9]
    mains, rests = scratch[9 : 9 + chunks], scratch[9 + chunks :]
    bands, slots = coef.shape[0], column.shape[0]
    inside = (count_here, slot_of, fixed, coef, column)
    copies = [
        pltpu.make_async_copy(src, to, done.at[i]) for i, (src, to) in enumerate(zip(refs, inside))
    ]
    for copy in copies:
        copy.start()
    for main, rest, count in zip(mains, rests, planes):
        if 2 * count * bands < main.shape[1]:
            main[...] = jnp.zeros_like(main)
            rest[...] = jnp.zeros_like(rest)

    def product(x, y, dims):
        return lax.dot_general(x, y, (dims, ((), ())), preferred_element_type=jnp.float32)

    copies[1].wait()
    copies[2].wait()
    held = slot_of[...].reshape(1, -1)
    at_pos = lax.broadcasted_iota(jnp.int32, (N, held.shape[1]), 0) == held
    at_pos = jnp.where(at_pos, 1.0, 0.0).astype(jnp.bfloat16)
    table = 0.0
    ordered = fixed.shape[0] // 2 - N
    for part in range(2):
        at = part * (N + ordered)
        pos = fixed[at : at + N]
        order = fixed[at + N : at + N + ordered, : held.shape[1]]
        rows_of_slot = product(at_pos, pos, ((0,), (0,))).astype(jnp.bfloat16)
        table = table + product(order, rows_of_slot, ((1,), (0,)))
    table = table.astype(jnp.bfloat16)

    stride = low.shape[0] // bands
    copies[3].wait()
    for s in range(slots):
        tile, shift = divmod(s * 2 * GB, LANES)
        x = coef[:, tile * LANES : (tile + 2) * LANES].astype(jnp.float32)
        if shift:
            x = pltpu.roll(x, 2 * LANES - shift, 1)
        low[pl.ds(s, bands, stride=stride), :] = x[:, :LANES]
        high[pl.ds(s, bands, stride=stride), :] = x[:, LANES:]

    for b in range(bands):
        here = slice(b * stride, b * stride + slots)
        x = jnp.concatenate([low[here], high[here]], axis=1).astype(jnp.bfloat16)
        x = jnp.concatenate([x[:LANES]] + [x[LANES:]] * 4, axis=0)
        val = product(table, x, ((1,), (1,)))
        at = 0
        for main, rest, count in zip(mains, rests, planes):
            for d in range(ranks):
                part = val[at : at + 2 * count]
                main[d, pl.ds(b, 2 * count, stride=bands), :] = part[:, :LANES]
                rest[d, pl.ds(b, 2 * count, stride=bands), :] = part[:, LANES:]
                at += up(2 * count, 8)

    copies[0].wait()
    copies[4].wait()
    c = column[...].reshape(1, -1).astype(jnp.float32)
    gx = jnp.floor((c + 0.5) * (1.0 / GB))
    row = lax.broadcasted_iota(jnp.int32, (INFO, slots), 0)
    live = count_here[0].astype(jnp.float32)
    info = jnp.where(row % 3 == 0, gx, jnp.where(row % 3 == 1, c - GB * gx, live))
    ends[...] = jnp.zeros_like(ends)
    ends[:, : slots - LANES] = info[:, LANES:]
    row = lax.broadcasted_iota(jnp.int32, (INFO, LANES), 0)
    info = jnp.where(row < 3, info[:, :LANES], jnp.where(row < 5, ends[...], 0.0))

    for c, (main, rest, count) in enumerate(zip(mains, rests, planes)):
        rows = 2 * count * bands
        span = main.shape[1] // GROUPS
        masks = lane_group(span, jnp.float32)
        at = rows + (INFO if c == 0 else 0)
        for k in range(ranks):
            out, d = (outs[0].at[k], k) if c == 0 else (outs[1 + (c - 1) * ranks + k], me ^ k)
            out[:rows, :] = main[d, :rows, :].astype(jnp.bfloat16)
            packed = rest[d, :span, :] * masks[0]
            for g in range(1, GROUPS):
                packed = packed + rest[d, g * span : (g + 1) * span, :] * masks[g]
            if c == 0:
                out[rows:at, :] = info.astype(jnp.bfloat16)
            out[at:, :] = packed.astype(jnp.bfloat16)


def plane_kernel(first, bands, ranks, planes, span, owners, own_rows, *refs):
    if first:
        recv, row_tab, end_tab, col_tab, weight, core, keep, send, turn, gx_of, gy_hot = refs[:11]
        blocks, source = [recv.at[src] for src in range(ranks)], lambda k: slice(k, k + 1)
    else:
        blocks, refs = refs[:ranks], refs[ranks - 1 :]
        _, row_tab, end_tab, col_tab, weight, core, turn, gx_of, gy_hot, keep, send = refs[:11]
        me = lax.axis_index("fft")
        source = lambda k: pl.ds(me ^ k, 1)
    lhs, pick, sticks, real, imag, both, half, tail, acc, acc_tail, share = refs[11:]
    live = planes * bands
    rows = 2 * live
    total = rows + INFO if first else rows
    cap = turn.shape[1]

    if first:
        place = lax.broadcasted_iota(jnp.int32, (1, cap), 1).astype(jnp.float32)
        start = jnp.zeros((1, 1), jnp.float32)
        for src in range(ranks):
            count = blocks[src][rows : rows + INFO, :].astype(jnp.float32)[2:3, 0:1]
            t = place - start
            turn[src : src + 1, :] = jnp.where(jnp.logical_and(t >= 0, t < count), t, -1.0)
            start = start + count

    masks = lane_group(span, jnp.bfloat16)
    k = lax.broadcasted_iota(jnp.int32, (2 * LANES, cap), 0)
    slot = jnp.where(k < LANES, k, LANES + k % 32).astype(jnp.float32).astype(jnp.bfloat16)
    one, zero = jnp.ones((), jnp.bfloat16), jnp.zeros((), jnp.bfloat16)
    if first:
        info_row = lax.broadcasted_iota(jnp.int32, (INFO, LANES), 0)
        info_main = (info_row < 3).astype(jnp.float32).astype(jnp.bfloat16)
    for src in range(ranks):
        at = src * 2 * LANES
        wanted = jnp.broadcast_to(turn[source(src), :].astype(jnp.bfloat16), slot.shape)
        pick[at : at + 2 * LANES, :] = jnp.where(slot == wanted, one, zero)
        block, low, high = blocks[src], slice(at, at + LANES), slice(at + LANES, at + 2 * LANES)
        lhs[:rows, low] = block[:rows, :]
        packed = block[total : total + span, :]
        for g in range(GROUPS):
            here = slice(g * span, min(rows, (g + 1) * span))
            if here.start < here.stop:
                lhs[here, high] = (packed * masks[g])[: here.stop - here.start]
        if first:
            info = block[rows:total, :]
            lhs[rows:, low] = info * info_main
            lhs[rows:, high] = info * (one - info_main)
    compact = jnp.dot(lhs[...], pick[...], preferred_element_type=jnp.float32)
    sticks[...] = compact[:rows].astype(jnp.bfloat16)

    if first:
        info = jnp.concatenate(
            [compact[rows:], jnp.zeros((LANES - INFO, cap), jnp.float32)], axis=0
        ).T
        lane = lax.broadcasted_iota(jnp.int32, (cap, LANES), 1).astype(jnp.float32)
        gx, gy = (info[:, i : i + 1] + info[:, i + 3 : i + 4] for i in range(2))
        gx_of[...] = jnp.broadcast_to(gx, (cap, LANES)).astype(jnp.bfloat16)
        gy_hot[...] = jnp.where(gy == lane, 1.0, 0.0).astype(jnp.bfloat16)

    def put(step, carry):
        for u in range(PAIRS):
            pair = PAIRS * step + u
            hot = []
            for side in range(2):
                gx = (2 * pair + side).astype(jnp.float32).astype(jnp.bfloat16)
                hot.append(jnp.where(gx_of[...] == gx, gy_hot[...], jnp.zeros((), jnp.bfloat16)))
            placed = jnp.dot(
                sticks[...], jnp.concatenate(hot, axis=1), preferred_element_type=jnp.float32
            )
            for side in range(2):
                lanes = slice(side * LANES, (side + 1) * LANES)
                at = 2 * pair + side
                real[pl.ds(at, live, stride=GB), :] = placed[:live, lanes]
                imag[pl.ds(at, live, stride=GB), :] = placed[live : 2 * live, lanes]
        return carry

    lax.fori_loop(0, GB // 2 // PAIRS, put, 0)

    acc[...] = jnp.zeros_like(acc)
    acc_tail[...] = jnp.zeros_like(acc_tail)

    def stacked(piece):
        return jnp.concatenate([piece[:, :LANES], piece[:, LANES:]], axis=0).astype(jnp.bfloat16)

    def rows_of(first_plane, count):
        for u in range(count):
            j = first_plane + u
            at = j * (bands * GB)
            at = at if isinstance(at, int) else pl.multiple_of(at, 8)
            at = pl.ds(at, bands * GB)
            x = jnp.concatenate(
                [real[at, :].astype(jnp.bfloat16), imag[at, :].astype(jnp.bfloat16)], axis=1
            )
            both[j] = x
            h = jnp.dot(x, row_tab[...], preferred_element_type=jnp.float32)
            for b in range(bands):
                half[j, b] = stacked(h[b * GB : (b + 1) * GB])

    deep = min(planes, 12)
    lax.fori_loop(0, planes // deep, lambda step, _: rows_of(step * deep, deep), None)
    rows_of(planes - planes % deep, planes % deep)

    tails = tail.shape[0]
    for t in range(tails):
        js = range(t * SHARE, min(planes, (t + 1) * SHARE))
        x = jnp.concatenate([both[j] for j in js], axis=1)
        h = jnp.dot(x, end_tab[: len(js) * 2 * LANES, :], preferred_element_type=jnp.float32)
        for b in range(bands):
            tail[t, b] = stacked(h[b * GB : (b + 1) * GB])

    wide = largest(bands, 12)

    def columns_of(step, carry):
        pieces = []
        for u in range(wide):
            b = wide * step + u
            pieces += [(acc, j, half, b) for j in range(planes)]
        for t in range(tails):
            pieces += [(acc_tail, t, tail, wide * step + u) for u in range(wide)]
        for i in range(0, len(pieces), 2):
            two = pieces[i : i + 2]
            x = jnp.concatenate([src[j, b] for _, j, src, b in two], axis=1)
            wave = jnp.dot(col_tab[...], x, preferred_element_type=jnp.float32)
            re, im = wave[:N], wave[N:]
            sq = re * re + im * im
            for side, (to, j, _, b) in enumerate(two):
                to[j] = to[j] + sq[:, side * LANES : (side + 1) * LANES] * weight[b]
        return carry

    lax.fori_loop(0, bands // wide, columns_of, 0)

    def deal(mine_bit):
        for o in range(owners):
            to = keep if o % 2 == mine_bit else send
            mine = slice(o * own_rows, (o + 1) * own_rows)
            pieces = [acc[j, mine, :] for j in range(planes)]
            pieces += [acc_tail[t, mine, :] for t in range(tails)]
            for i, piece in enumerate(pieces):
                share[i * own_rows : (i + 1) * own_rows, :] = piece
            to[o // 2] = share[...].astype(jnp.bfloat16)

    if share.shape[0] > (planes + tails) * own_rows:
        share[...] = jnp.zeros_like(share)

    @pl.when(core[0] == 0)
    def _():
        deal(0)

    @pl.when(core[0] != 0)
    def _():
        deal(1)


def sum_kernel(planes, own_rows, *refs):
    *parts, out = refs
    base = 0
    for c, count in enumerate(planes):
        total = parts[2 * c][...].astype(jnp.float32) + parts[2 * c + 1][...].astype(jnp.float32)
        for j in range(count):
            at = j % SHARE * TAIL
            main, end = (i * own_rows for i in (j, count + j // SHARE))
            out[base + j, :, :LANES] = total[main : main + own_rows]
            out[base + j, :, LANES:] = total[end : end + own_rows, at : at + TAIL]
        base += count


def up(n, m):
    return -(-n // m) * m


def largest(n, most):
    return max(d for d in range(1, most + 1) if n % d == 0)


def vmem_call(kernel, out_shape, n_in, scratch=(), flops=1, smem=(), far=()):
    vmem_scratch = [m for m in scratch if m.memory_space == pltpu.VMEM]
    used = sum(math.prod(m.shape) * jnp.dtype(m.dtype).itemsize for m in vmem_scratch)
    vmem = pl.BlockSpec(memory_space=pltpu.VMEM)
    scalar = pl.BlockSpec(memory_space=pltpu.SMEM)
    hbm = pl.BlockSpec(memory_space=pltpu.HBM)
    many = isinstance(out_shape, list)
    return pl.pallas_call(
        kernel,
        out_shape=out_shape,
        in_specs=[scalar if i in smem else hbm if i in far else vmem for i in range(n_in)],
        out_specs=[vmem] * len(out_shape) if many else vmem,
        scratch_shapes=list(scratch),
        compiler_params=pltpu.CompilerParams(vmem_limit_bytes=min(62 * 2**20, used + 12 * 2**20)),
        cost_estimate=pl.CostEstimate(flops=flops, bytes_accessed=1 << 20, transcendentals=0),
    )


def partners(axis, bit):
    return [(i, i ^ (1 << bit)) for i in range(lax.axis_size(axis))]


def halve(keep, send, axis):
    bit = 0
    while True:
        got = lax.ppermute(send, axis, partners(axis, bit))
        if keep.shape[0] == 1:
            return keep[0], got[0]
        whole = (keep.astype(jnp.float32) + got.astype(jnp.float32)).astype(keep.dtype)
        bit += 1
        here = lax.axis_index(axis) >> bit & 1
        pairs = whole.reshape((whole.shape[0] // 2, 2) + whole.shape[1:])
        keep = lax.dynamic_index_in_dim(pairs, here, 1, keepdims=False)
        send = lax.dynamic_index_in_dim(pairs, 1 - here, 1, keepdims=False)


def shards(coefficients, occupations, columns, counts, plane_slot):
    bands = coefficients.shape[0]
    ranks = lax.axis_size("fft")
    owners = lax.axis_size("band")
    slots = columns.shape[0]
    held = plane_slot.shape[0] // ranks
    planes = (held // 3, held - held // 3)
    cap = up(ranks * slots * 2 // 5, LANES)
    own_rows = N // owners
    bf16, f32 = jnp.bfloat16, jnp.float32

    weight = occupations / (bands * owners)
    core = (lax.axis_index("band") & 1)[None]
    tables = wave_tables()

    spans = [up(-(-2 * count * bands // GROUPS), 8) for count in planes]
    rows = [2 * count * bands for count in planes]
    fixed = stick_constants(planes, ranks)
    stride = up(slots, 8) + 8
    outgoing = vmem_call(
        functools.partial(stick_kernel, planes, ranks),
        [jax.ShapeDtypeStruct((ranks, rows[0] + spans[0] + INFO, LANES), bf16)]
        + [jax.ShapeDtypeStruct((rows[1] + spans[1], LANES), bf16)] * ranks,
        5,
        [
            pltpu.SMEM(counts.shape, jnp.int32),
            pltpu.VMEM(plane_slot.shape, jnp.int32),
            pltpu.VMEM(fixed.shape, bf16),
            pltpu.VMEM(coefficients.shape, bf16),
            pltpu.VMEM(columns.shape, jnp.int32),
            pltpu.SemaphoreType.DMA((5,)),
        ]
        + [pltpu.VMEM((bands * stride, LANES), f32)] * 2
        + [pltpu.VMEM((INFO, LANES), f32)]
        + [pltpu.VMEM((ranks, GROUPS * span, LANES), f32) for span in spans * 2],
        flops=4 * 10**9,
        far=range(5),
    )(counts, *[pltpu.with_memory_space_constraint(x, pltpu.HBM) for x in (plane_slot, fixed, coefficients, columns)])
    kept_shapes = [
        jax.ShapeDtypeStruct((ranks, cap), f32),
        jax.ShapeDtypeStruct((cap, LANES), bf16),
        jax.ShapeDtypeStruct((cap, LANES), bf16),
    ]
    kept, halves = [], []
    for c, (count, span) in enumerate(zip(planes, spans)):
        first = c == 0
        if first:
            received = [lax.all_to_all(outgoing[0], "fft", split_axis=0, concat_axis=0, tiled=True)]
        else:
            received = [outgoing[1]]
            for k in range(1, ranks):
                pairs = [(i, i ^ k) for i in range(ranks)]
                received.append(lax.ppermute(outgoing[1 + k], "fft", pairs))
        tails = -(-count // SHARE)
        dealt = up((count + tails) * own_rows, 8)
        dens_shape = jax.ShapeDtypeStruct((owners // 2, dealt, LANES), bf16)
        run = vmem_call(
            functools.partial(plane_kernel, first, bands, ranks, count, span, owners, own_rows),
            [dens_shape] * 2 + (kept_shapes if first else []),
            len(received) + (5 if first else 8),
            [
                pltpu.VMEM((rows[c] + (INFO if first else 0), ranks * 2 * LANES), bf16),
                pltpu.VMEM((ranks * 2 * LANES, cap), bf16),
                pltpu.VMEM((rows[c], cap), bf16),
                pltpu.VMEM((count * bands * GB, LANES), f32),
                pltpu.VMEM((count * bands * GB, LANES), f32),
                pltpu.VMEM((count, bands * GB, 2 * LANES), bf16),
                pltpu.VMEM((count, bands, 2 * GB, LANES), bf16),
                pltpu.VMEM((tails, bands, 2 * GB, LANES), bf16),
                pltpu.VMEM((count, N, LANES), f32),
                pltpu.VMEM((tails, N, LANES), f32),
                pltpu.VMEM((dealt, LANES), f32),
            ],
            flops=16 * 10**9,
            smem=(len(received) + 3, len(received) + 4),
        )
        results = run(*received, *tables, weight, core, *kept)
        if first:
            kept = list(results[2:])
        halves += halve(results[0], results[1], "band")
    return vmem_call(
        functools.partial(sum_kernel, planes, own_rows),
        jax.ShapeDtypeStruct((held, own_rows, N), f32),
        len(halves),
    )(*halves)


def solution(mesh):
    placed = (P("band", "fft"), P("band"), P("fft"), P("fft"), P())

    return jax.shard_map(
        shards, mesh=mesh, in_specs=placed, out_specs=P("fft", "band", None), check_vma=False
    )
```
